32 devices in a mesh: dp: 4 (over z), col: 2 (over y), fsdp: 4 (over x, core).
Axes of the slice: x: 2, y: 2, z: 4, core: 2. Of those that a mesh axis runs over, the one named last changes fastest.
Arguments:
- x_act: bfloat16 [98304, 576], P(('dp', 'col', 'fsdp'))
- dy_out: bfloat16 [98304, 576], P(('dp', 'col', 'fsdp'))
- w_gate: bfloat16 [576, 1536], P(None, ('col', 'fsdp'))
- w_up: bfloat16 [576, 1536], P(None, ('col', 'fsdp'))
- w_down: bfloat16 [1536, 576], P(('col', 'fsdp'))
- v_gate: bfloat16 [576, 1536], P(None, ('col', 'fsdp'))
- v_up: bfloat16 [576, 1536], P(None, ('col', 'fsdp'))
- v_down: bfloat16 [1536, 576], P(('col', 'fsdp'))
- g_next: float32 [32, 3, 576, 1536], P(('dp', 'col', 'fsdp'))
Outputs:
- output 1: bfloat16 [98304, 576], P(('dp', 'col', 'fsdp'))
- output 2: float32 [3, 576, 1536], P(None, None, ('col', 'fsdp'))
- output 3: float32 [32, 3, 576, 1536], P(('dp', 'col', 'fsdp'))
- output 4: bfloat16 [576, 1536], replicated
- output 5: bfloat16 [576, 1536], replicated
- output 6: bfloat16 [1536, 576], replicated
All inputs are finite; a program needn't handle non-finite values.
Results may differ from the reference program's by a relative error of at most 0.0105829.
Values are sent between devices in bfloat16 or wider.
A program may use at most 1 GiB of HBM per device.

```python
import jax
import jax.numpy as jnp
from jax import lax

D_MODEL = 576
D_FF = 1536
TOKENS_DEV = 3072
N_DEVICES = 32


def draw_normal(key, shape, scaling):
    return jax.random.normal(key, shape, jnp.float32) * scaling


def setup_inputs(seed: int = 0) -> dict:
    keys = jax.random.split(jax.random.key(seed), 9)
    all_rows = N_DEVICES * TOKENS_DEV
    model_scale = D_MODEL ** -0.5
    hidden_scale = D_FF ** -0.5
    return {
        'x_act': draw_normal(keys[0], (all_rows, D_MODEL), 1.0).astype(jnp.bfloat16),
        'dy_out': draw_normal(keys[1], (all_rows, D_MODEL), 1.0).astype(jnp.bfloat16),
        'w_gate': draw_normal(keys[2], (D_MODEL, D_FF), model_scale).astype(jnp.bfloat16),
        'w_up': draw_normal(keys[3], (D_MODEL, D_FF), model_scale).astype(jnp.bfloat16),
        'w_down': draw_normal(keys[4], (D_FF, D_MODEL), hidden_scale).astype(jnp.bfloat16),
        'v_gate': draw_normal(keys[5], (D_MODEL, D_FF), model_scale).astype(jnp.bfloat16),
        'v_up': draw_normal(keys[6], (D_MODEL, D_FF), model_scale).astype(jnp.bfloat16),
        'v_down': draw_normal(keys[7], (D_FF, D_MODEL), hidden_scale).astype(jnp.bfloat16),
        'g_next': draw_normal(keys[8], (N_DEVICES, 3, D_MODEL, D_FF), 1.0),
    }


def reference(x_act, dy_out, w_gate, w_up, w_down, v_gate, v_up, v_down, g_next):
    x_dev = x_act.reshape(N_DEVICES, TOKENS_DEV, D_MODEL)
    dy_dev = dy_out.reshape(N_DEVICES, TOKENS_DEV, D_MODEL)

    def one_device(operands):
        x_loc, dy_loc = operands
        pre_gate = jnp.dot(x_loc, w_gate, preferred_element_type=jnp.float32)
        pre_up = jnp.dot(x_loc, w_up, preferred_element_type=jnp.float32)
        sig_gate = jax.nn.sigmoid(pre_gate)
        act_gate = pre_gate * sig_gate
        hidden = (act_gate * pre_up).astype(jnp.bfloat16)
        d_hidden = jnp.dot(dy_loc, w_down.T, preferred_element_type=jnp.float32)
        d_gate = (d_hidden * pre_up * sig_gate * (1.0 + pre_gate * (1.0 - sig_gate))).astype(jnp.bfloat16)
        d_up = (d_hidden * act_gate).astype(jnp.bfloat16)
        dx_loc = (jnp.dot(d_gate, w_gate.T, preferred_element_type=jnp.float32)
                  + jnp.dot(d_up, w_up.T, preferred_element_type=jnp.float32)).astype(jnp.bfloat16)
        grad_gate = jnp.dot(x_loc.T, d_gate, preferred_element_type=jnp.float32)
        grad_up = jnp.dot(x_loc.T, d_up, preferred_element_type=jnp.float32)
        grad_down_t = jnp.dot(dy_loc.T, hidden, preferred_element_type=jnp.float32)
        return dx_loc, jnp.stack([grad_gate, grad_up, grad_down_t])

    dx_dev, dw_local = lax.map(one_device, (x_dev, dy_dev))
    dx_in = dx_dev.reshape(N_DEVICES * TOKENS_DEV, D_MODEL)
    dw_next = jnp.sum(g_next.astype(jnp.bfloat16).astype(jnp.float32), axis=0)
    return dx_in, dw_next, dw_local, v_gate, v_up, v_down
```

```python
import functools

import jax
import jax.numpy as jnp
from jax import lax
from jax.experimental import pallas as pl
from jax.experimental.pallas import tpu as pltpu
from jax.sharding import PartitionSpec as P

ALL_AXES = ('dp', 'col', 'fsdp')
FSDP_AXES = ('col', 'fsdp')
MESH = pl.DeviceIdType.MESH

D = 576
F = 1536
N = 3072
T = 512
NT = N // T
SH = 192
FC = 384
RT = 144
HR = D // 2
QR = HR // 2
NN = (((1,), (0,)), ((), ()))
NTD = (((1,), (1,)), ((), ()))

STEPS = {
    'A': (0, 1, 2), 'W3': (15,), 'V': (3,),
    'B': (4, 6, 9), 'C': (8, 11, 13),
    'D0': (9, 12, 14), 'D1': (10, 13, 15), 'E0': (12, 15, 18), 'E1': (13, 16, 19),
    'V1': (20,), 'V2': (21,),
}


def dot(a, b, dn=NN):
    return lax.dot_general(a, b, dn, preferred_element_type=jnp.float32)


def kernel(xt, dyt, w1, w3, w2, v1, v3, v2, g, dxt, dw, vo, gs,
           xs, ys, pair, blk, vblk, wt, dxa, dwa, dab, hb, dxs,
           gf, gb, gp, r1, p2, r2, rr, z1, z2, zs, tt,
           s_tok, s_loc, s_g, s_dw, s_dx, s_vo, s_t, ss, rs):
    z = lax.axis_index('dp')
    y = lax.axis_index('col')
    f = lax.axis_index('fsdp')
    x = f // 2
    k = f % 2
    own = 2 * y + x
    partner = (z, y, f + 1 - 2 * k)
    xn = (z, y, (f + 2) % 4)
    yn = (z, 1 - y, f)
    z_pair = z + 1 - 2 * (z % 2)
    zp = (z_pair, y, f)
    zm = (3 - z, y, f)
    at_end = (z == 0) | (z == 3)
    inner = (z == 1) | (z == 2)

    def rcopy(n, src, dst, dev):
        return pltpu.make_async_remote_copy(
            src_ref=src, dst_ref=dst, send_sem=ss.at[n], recv_sem=rs.at[n], device_id=dev, device_id_type=MESH)

    def tok(t):
        cols = pl.ds(pl.multiple_of(t * T, T), T)
        return (pltpu.make_async_copy(xt.at[:, cols], xs.at[t], s_tok.at[0, t]),
                pltpu.make_async_copy(dyt.at[:, cols], ys.at[t], s_tok.at[1, t]))

    def gload(i, half):
        r0 = pl.multiple_of(half * (6 * RT) + i * RT, RT)
        return pltpu.make_async_copy(g.at[pl.ds(r0, RT), :], gf.at[i], s_g.at[i])

    shards = ((w1, w3, w2), (v1, v3, v2))
    myrows = pl.ds(pl.multiple_of(k * SH, SH), SH)
    local_shards = [pltpu.make_async_copy(shards[u][m], pair.at[u, m, myrows, :], s_loc.at[3 * u + m])
                    for u in range(2) for m in range(3)]
    for i in range(6):
        gload(i, 1 - k).start()
    for c in local_shards:
        c.start()

    bar = pltpu.get_barrier_semaphore()
    for dev in (partner, xn, yn, zp, zm):
        pl.semaphore_signal(bar, inc=1, device_id=dev, device_id_type=MESH)
    pl.semaphore_wait(bar, 5)

    to_pair = [rcopy(3 * u + m, shards[u][m], pair.at[u, m, myrows, :], partner) for u in range(2) for m in range(3)]
    half = pl.ds(pl.multiple_of(k * HR, HR), HR)
    other = pl.ds(pl.multiple_of((1 - k) * HR, HR), HR)
    qa = pl.ds(pl.multiple_of(k * HR, QR), QR)
    qb = pl.ds(pl.multiple_of(k * HR + QR, QR), QR)

    def blkcols(cx, cy):
        xx = 1 - x if cx else x
        yy = 1 - y if cy else y
        return pl.ds(pl.multiple_of((2 * yy + xx) * FC, FC), FC)

    w_x = rcopy(6, blk.at[0, :, half, :], blk.at[1, :, half, :], xn)
    w_y = rcopy(7, blk.at[0, :, half, :], blk.at[2, :, half, :], yn)
    w_f1 = rcopy(8, blk.at[1, :, half, :], blk.at[1, :, half, :], partner)
    w_f2 = rcopy(9, blk.at[2, :, half, :], blk.at[2, :, half, :], partner)
    w_da = rcopy(10, blk.at[1, :, qa, :], blk.at[3, :, qa, :], yn)
    w_db = rcopy(11, blk.at[2, :, qb, :], blk.at[3, :, qb, :], xn)
    w_f3 = rcopy(12, blk.at[3, :, half, :], blk.at[3, :, half, :], partner)

    v_own = pltpu.make_async_copy(vblk, vo.at[:, :, blkcols(0, 0)], s_vo)
    v_x = rcopy(13, vblk.at[:, half, :], vo.at[:, half, blkcols(0, 0)], xn)
    v_y = rcopy(14, vblk.at[:, half, :], vo.at[:, half, blkcols(0, 0)], yn)
    v_f1 = rcopy(15, vo.at[:, half, blkcols(1, 0)], vo.at[:, half, blkcols(1, 0)], partner)
    v_f2 = rcopy(16, vo.at[:, half, blkcols(0, 1)], vo.at[:, half, blkcols(0, 1)], partner)
    v_da = rcopy(17, vo.at[:, qa, blkcols(1, 0)], vo.at[:, qa, blkcols(1, 0)], yn)
    v_db = rcopy(18, vo.at[:, qb, blkcols(0, 1)], vo.at[:, qb, blkcols(0, 1)], xn)
    v_f3 = rcopy(19, vo.at[:, half, blkcols(1, 1)], vo.at[:, half, blkcols(1, 1)], partner)

    def to_partner(i):
        return rcopy(20 + i, gb.at[i], gp.at[i], partner)

    def first_x(j, yy):
        return rcopy(26 + 2 * j + yy, gp.at[j, 2 * yy + 1 - x], r1.at[j, yy], xn)

    def first_y(j, xx):
        return rcopy(32 + 2 * j + xx, gp.at[3 + j, 2 * (1 - y) + xx], r1.at[3 + j, xx], yn)

    def second_y(j):
        return rcopy(38 + j, p2.at[j, 1 - y], r2.at[j], yn)

    def second_x(j):
        return rcopy(41 + j, p2.at[3 + j, 1 - x], r2.at[3 + j], xn)

    def z_in(i):
        return rcopy(44 + i, rr.at[i], z1.at[i], zp)

    def z_mid(i):
        return rcopy(50 + i, zs.at[i], z2.at[i], zm)

    def z_out(i):
        return rcopy(56 + i, tt.at[i], tt.at[i], zp)

    def t_pair(i):
        return rcopy(62 + i, tt.at[i], gs.at[k, i], partner)

    def t_own(i):
        return pltpu.make_async_copy(tt.at[i], gs.at[k, i], s_t.at[i])

    for c in to_pair:
        c.start()
    for t in range(NT):
        for c in tok(t):
            c.start()

    def send_half(i, _):
        gload(i, 1 - k).wait()
        for q in range(4):
            gb[i, q] = gf[i, :, q * FC:(q + 1) * FC].astype(jnp.bfloat16)
        to_partner(i).start()
        gload(i, k).start()
        return 0

    lax.fori_loop(0, 6, send_half, 0)

    for m in range(3):
        local_shards[m].wait()
        to_pair[m].wait_recv()
        blk[0, m] = pair[0, m].T
    w_x.start()
    w_y.start()

    def own_tile(i):
        gload(i, k).wait()
        to_partner(i).wait_recv()
        for q in range(4):
            gp[i, q] = (gp[i, q].astype(jnp.float32)
                        + gf[i, :, q * FC:(q + 1) * FC].astype(jnp.bfloat16).astype(jnp.float32)).astype(jnp.bfloat16)

    def stage_a(j):
        own_tile(j)
        own_tile(3 + j)
        for b in range(2):
            first_x(j, b).start()
            first_y(j, b).start()

    def stage_b(j):
        for b in range(2):
            first_x(j, b).wait_recv()
            p2[j, b] = (gp[j, 2 * b + x].astype(jnp.float32) + r1[j, b].astype(jnp.float32)).astype(jnp.bfloat16)
            first_y(j, b).wait_recv()
            p2[3 + j, b] = (gp[3 + j, 2 * y + b].astype(jnp.float32)
                            + r1[3 + j, b].astype(jnp.float32)).astype(jnp.bfloat16)
        second_y(j).start()
        second_x(j).start()

    def stage_c(j):
        second_y(j).wait_recv()
        rr[j] = p2[j, y].astype(jnp.float32) + r2[j].astype(jnp.float32)
        second_x(j).wait_recv()
        rr[3 + j] = p2[3 + j, x].astype(jnp.float32) + r2[3 + j].astype(jnp.float32)

        @pl.when(at_end)
        def _():
            z_in(j).start()
            z_in(3 + j).start()

    def stage_d(i):
        @pl.when(inner)
        def _():
            z_in(i).wait_recv()
            zs[i] = rr[i] + z1[i]
            z_mid(i).start()

    def stage_e(i):
        @pl.when(inner)
        def _():
            z_mid(i).wait_recv()
            tt[i] = zs[i] + z2[i]
            z_out(i).start()
            t_pair(i).start()
            t_own(i).start()

    def v_start():
        for m in range(3):
            local_shards[3 + m].wait()
            to_pair[3 + m].wait_recv()
            vblk[m] = pair[1, m].T
        v_own.start()
        v_x.start()
        v_y.start()

    def w_1():
        w_x.wait_recv()
        w_f1.start()
        w_da.start()

    def w_2():
        w_y.wait_recv()
        w_f2.start()
        w_db.start()

    def w_3():
        w_da.wait_recv()
        w_db.wait_recv()
        w_f3.start()

    def v_1():
        v_x.wait_recv()
        v_f1.start()
        v_da.start()

    def v_2():
        v_y.wait_recv()
        v_f2.start()
        v_db.start()

    stages = {
        'A': stage_a, 'B': stage_b, 'C': stage_c,
        'D0': stage_d, 'D1': lambda j: stage_d(3 + j), 'E0': stage_e, 'E1': lambda j: stage_e(3 + j),
        'V': lambda j: v_start(), 'W3': lambda j: w_3(),
        'V1': lambda j: v_1(), 'V2': lambda j: v_2(),
    }
    order = ('W3', 'A', 'B', 'C', 'D0', 'D1', 'E0', 'E1', 'V', 'V1', 'V2')

    def tick(step):
        for name in order:
            for j, n in enumerate(STEPS[name]):
                if n < 24:
                    pl.when(step == n)(functools.partial(stages[name], j))

    def dw_out(c):
        cx, cy = c % 2, c // 2
        q = 2 * (y + cy - 2 * y * cy) + x + cx - 2 * x * cx
        return pltpu.make_async_copy(dwa, dw.at[:, :, pl.ds(pl.multiple_of(q * FC, FC), FC)], s_dw)

    def chunk(c, _):
        @pl.when(c == 1)
        def _():
            w_1()
            w_2()
            w_f1.wait_recv()

        @pl.when(c == 2)
        def _():
            w_f2.wait_recv()

        @pl.when(c == 3)
        def _():
            w_f3.wait_recv()

        for m in range(3):
            wt[m * FC:(m + 1) * FC, :] = blk[c, m].T

        @pl.when(c > 0)
        def _():
            dw_out(c - 1).wait()

        dwa[...] = jnp.zeros_like(dwa)

        def tile(t, _):
            step = c * NT + t

            @pl.when(c == 0)
            def _():
                for cp in tok(t):
                    cp.wait()
                dxa[t] = jnp.zeros((D, T), jnp.float32)

            tick(step)
            xv = xs[t]
            yv = ys[t]
            a = dot(wt[0:FC, :], xv)
            b = dot(wt[FC:2 * FC, :], xv)
            dh = dot(wt[2 * FC:3 * FC, :], yv)
            sg = jnp.tanh(a * 0.5) * 0.5 + 0.5
            act = a * sg
            hb[...] = (act * b).astype(jnp.bfloat16)
            dab[FC:, :] = (dh * act).astype(jnp.bfloat16)
            dab[:FC, :] = (dh * b * (sg + act * (1.0 - sg))).astype(jnp.bfloat16)
            dxa[t] += dot(blk[c, 0], dab[:FC, :]) + dot(blk[c, 1], dab[FC:, :])
            gw = dot(xv, dab[...], NTD)
            dwa[0] += gw[:, :FC]
            dwa[1] += gw[:, FC:]
            dwa[2] += dot(yv, hb[...], NTD)
            return 0

        lax.fori_loop(0, NT, tile, 0)
        dw_out(c).start()
        return 0

    lax.fori_loop(0, 4, chunk, 0)

    def dx_out(t):
        return pltpu.make_async_copy(dxs.at[t % 2], dxt.at[:, pl.ds(pl.multiple_of(t * T, T), T)], s_dx.at[t % 2])

    def write_dx(t, _):
        @pl.when(t >= 2)
        def _():
            dx_out(t - 2).wait()

        dxs[t % 2] = dxa[t].astype(jnp.bfloat16)
        dx_out(t).start()
        return 0

    lax.fori_loop(0, NT, write_dx, 0)

    for name in order:
        for j, n in enumerate(STEPS[name]):
            if n >= 24:
                stages[name](j)

    for i in range(6):
        @pl.when(at_end)
        def _():
            z_out(i).wait_recv()
            t_pair(i).start()
            t_own(i).start()
    v_da.wait_recv()
    v_db.wait_recv()
    v_f3.start()

    dw_out(3).wait()
    dx_out(NT - 2).wait()
    dx_out(NT - 1).wait()
    v_own.wait()
    for i in range(6):
        t_own(i).wait()
        t_pair(i).wait()
        to_partner(i).wait_send()

        @pl.when(at_end)
        def _():
            z_in(i).wait_send()

        @pl.when(inner)
        def _():
            z_mid(i).wait_send()
            z_out(i).wait_send()
    for j in range(3):
        for b in range(2):
            first_x(j, b).wait_send()
            first_y(j, b).wait_send()
        second_x(j).wait_send()
        second_y(j).wait_send()
    for c in to_pair:
        c.wait_send()
    for c in (w_x, w_y, w_f1, w_f2, w_da, w_db, w_f3, v_x, v_y, v_f1, v_f2, v_da, v_db, v_f3):
        c.wait_send()
    for c in (v_f1, v_f2, v_f3):
        c.wait_recv()


def step_kernel(xt, dyt, w1, w3, w2, v1, v3, v2, g):
    any_spec = pl.BlockSpec(memory_space=pl.ANY)
    bf, f32 = jnp.bfloat16, jnp.float32
    V = pltpu.VMEM
    dma = pltpu.SemaphoreType.DMA
    return pl.pallas_call(
        kernel,
        name='mlp_step',
        out_shape=(jax.ShapeDtypeStruct((D, N), bf), jax.ShapeDtypeStruct((3, D, F), f32),
                   jax.ShapeDtypeStruct((3, D, F), bf), jax.ShapeDtypeStruct((2, 6, RT, FC), f32)),
        in_specs=[any_spec] * 9,
        out_specs=(any_spec,) * 4,
        scratch_shapes=[
            V((NT, D, T), bf), V((NT, D, T), bf), V((2, 3, FC, D), bf), V((4, 3, D, FC), bf), V((3, D, FC), bf),
            V((3 * FC, D), bf), V((NT, D, T), f32), V((3, D, FC), f32), V((2 * FC, T), bf), V((FC, T), bf),
            V((2, D, T), bf),
            V((6, RT, F), f32), V((6, 4, RT, FC), bf), V((6, 4, RT, FC), bf), V((6, 2, RT, FC), bf),
            V((6, 2, RT, FC), bf), V((6, RT, FC), bf), V((6, RT, FC), f32), V((6, RT, FC), f32),
            V((6, RT, FC), f32), V((6, RT, FC), f32), V((6, RT, FC), f32),
            dma((2, NT)), dma((6,)), dma((6,)), dma, dma((2,)), dma, dma((6,)), dma((68,)), dma((68,)),
        ],
        compiler_params=pltpu.CompilerParams(
            collective_id=0, has_side_effects=True, vmem_limit_bytes=67_000_000),
        cost_estimate=pl.CostEstimate(flops=43_500_000_000, bytes_accessed=60_000_000, transcendentals=4_718_592),
    )(xt, dyt, w1, w3, w2, v1, v3, v2, g)


def solution(mesh):
    def device_step(x_loc, dy_loc, w_gate, w_up, w_down, v_gate, v_up, v_down, g_next):
        dxt, dw, vo, gs = step_kernel(
            x_loc.T, dy_loc.T, w_gate.T, w_up.T, w_down, v_gate.T, v_up.T, v_down, g_next.reshape(3 * D, F))
        core = lax.axis_index('fsdp') % 2
        grad = lax.dynamic_slice_in_dim(gs.reshape(3, D, FC), core * SH, SH, axis=2)
        return dxt.T, grad, dw[None], vo[0], vo[1], vo[2].T

    row_spec = P(ALL_AXES, None)
    col_shard = P(None, FSDP_AXES)
    row_shard = P(FSDP_AXES, None)
    dev_spec = P(ALL_AXES, None, None, None)
    return jax.shard_map(
        device_step, mesh=mesh,
        in_specs=(row_spec, row_spec, col_shard, col_shard, row_shard, col_shard, col_shard, row_shard, dev_spec),
        out_specs=(row_spec, P(None, None, FSDP_AXES), dev_spec, P(), P(), P()),
        check_vma=False)
```

```python
import functools

import jax
import jax.numpy as jnp
from jax import lax
from jax.experimental import pallas as pl
from jax.experimental.pallas import tpu as pltpu
from jax.sharding import PartitionSpec as P

ALL_AXES = ('dp', 'col', 'fsdp')
FSDP_AXES = ('col', 'fsdp')
MESH = pl.DeviceIdType.MESH

D = 576
F = 1536
N = 3072
T = 512
NT = N // T
SH = 192
FC = 384
RT = 144
HR = D // 2
QR = HR // 2
NN = (((1,), (0,)), ((), ()))
NTD = (((1,), (1,)), ((), ()))

STEPS = {
    'A': (0, 1, 6), 'W1': (4,), 'WZ': (9,), 'WD': (12,), 'W3': (16,), 'V': (13,), 'V1': (20, 22, 24),
    'B': (6, 7, 10), 'C': (8, 11, 12),
    'D0': (10, 14, 17), 'D1': (12, 16, 19), 'E0': (14, 18, 22), 'E1': (16, 20, 24),
}


def dot(a, b, dn=NN):
    return lax.dot_general(a, b, dn, preferred_element_type=jnp.float32)


def kernel(xt, dyt, w1, w3, w2, v1, v3, v2, g, dxt, dw, vo, gs,
           xs, ys, pair, blk, vblk, wt, dxa, dwa, dab, hb, dxs,
           gf, gb, gp, r1, p2, r2, rb, z1, z2, zs, tt, to,
           s_tok, s_loc, s_g, s_dw, s_dx, s_vo, s_t, ss, rs):
    z = lax.axis_index('dp')
    y = lax.axis_index('col')
    f = lax.axis_index('fsdp')
    x = f // 2
    k = f % 2
    own = 2 * y + x
    partner = (z, y, f + 1 - 2 * k)
    xn = (z, y, (f + 2) % 4)
    yn = (z, 1 - y, f)
    z_pair = z + 1 - 2 * (z % 2)
    zp = (z_pair, y, f)
    zm = (3 - z, y, f)
    at_end = (z == 0) | (z == 3)
    inner = (z == 1) | (z == 2)

    def rcopy(n, src, dst, dev):
        return pltpu.make_async_remote_copy(
            src_ref=src, dst_ref=dst, send_sem=ss.at[n], recv_sem=rs.at[n], device_id=dev, device_id_type=MESH)

    def tok(t):
        cols = pl.ds(pl.multiple_of(t * T, T), T)
        return (pltpu.make_async_copy(xt.at[:, cols], xs.at[t], s_tok.at[0, t]),
                pltpu.make_async_copy(dyt.at[:, cols], ys.at[t], s_tok.at[1, t]))

    def gload(i, half):
        r0 = pl.multiple_of(half * (6 * RT) + i * RT, RT)
        return pltpu.make_async_copy(g.at[pl.ds(r0, RT), :], gf.at[i], s_g.at[i])

    shards = ((w1, w3, w2), (v1, v3, v2))
    myrows = pl.ds(pl.multiple_of(k * SH, SH), SH)
    local_shards = [pltpu.make_async_copy(shards[u][m], pair.at[u, m, myrows, :], s_loc.at[3 * u + m])
                    for u in range(2) for m in range(3)]
    for i in range(6):
        gload(i, 1 - k).start()
    for c in local_shards:
        c.start()

    bar = pltpu.get_barrier_semaphore()
    for dev in (partner, xn, yn, zp, zm):
        pl.semaphore_signal(bar, inc=1, device_id=dev, device_id_type=MESH)
    pl.semaphore_wait(bar, 5)

    to_pair = [rcopy(3 * u + m, shards[u][m], pair.at[u, m, myrows, :], partner) for u in range(2) for m in range(3)]
    half = pl.ds(pl.multiple_of(k * HR, HR), HR)
    other = pl.ds(pl.multiple_of((1 - k) * HR, HR), HR)
    qa = pl.ds(pl.multiple_of(k * HR, QR), QR)
    qb = pl.ds(pl.multiple_of(k * HR + QR, QR), QR)

    def blkcols(cx, cy):
        xx = 1 - x if cx else x
        yy = 1 - y if cy else y
        return pl.ds(pl.multiple_of((2 * yy + xx) * FC, FC), FC)

    zo = z % 2
    qm = pl.ds(pl.multiple_of(k * HR + zo * QR, QR), QR)
    qo = pl.ds(pl.multiple_of(k * HR + (1 - zo) * QR, QR), QR)
    w_x = rcopy(6, blk.at[0, :, qm, :], blk.at[1, :, qm, :], xn)
    w_y = rcopy(7, blk.at[0, :, qm, :], blk.at[2, :, qm, :], yn)
    w_zx = rcopy(8, blk.at[1, :, qm, :], blk.at[1, :, qm, :], zp)
    w_zy = rcopy(9, blk.at[2, :, qm, :], blk.at[2, :, qm, :], zp)
    w_f1a = rcopy(62, blk.at[1, :, qm, :], blk.at[1, :, qm, :], partner)
    w_f1b = rcopy(63, blk.at[1, :, qo, :], blk.at[1, :, qo, :], partner)
    w_f2a = rcopy(64, blk.at[2, :, qm, :], blk.at[2, :, qm, :], partner)
    w_f2b = rcopy(65, blk.at[2, :, qo, :], blk.at[2, :, qo, :], partner)
    w_da = rcopy(10, blk.at[1, :, qa, :], blk.at[3, :, qa, :], yn)
    w_db = rcopy(11, blk.at[2, :, qb, :], blk.at[3, :, qb, :], xn)
    w_f3 = rcopy(12, blk.at[3, :, half, :], blk.at[3, :, half, :], partner)

    v_own = pltpu.make_async_copy(vblk, vo.at[:, :, blkcols(0, 0)], s_vo)
    def v_copies(m):
        n = 66 + 7 * m
        q0, q1, q2, q3 = blkcols(0, 0), blkcols(1, 0), blkcols(0, 1), blkcols(1, 1)
        return (rcopy(n, vblk.at[m, half, :], vo.at[m, half, q0], xn),
                rcopy(n + 1, vblk.at[m, half, :], vo.at[m, half, q0], yn),
                rcopy(n + 2, vo.at[m, half, q1], vo.at[m, half, q1], partner),
                rcopy(n + 3, vo.at[m, half, q2], vo.at[m, half, q2], partner),
                rcopy(n + 4, vo.at[m, qa, q1], vo.at[m, qa, q1], yn),
                rcopy(n + 5, vo.at[m, qb, q2], vo.at[m, qb, q2], xn),
                rcopy(n + 6, vo.at[m, half, q3], vo.at[m, half, q3], partner))

    def to_partner(i):
        return rcopy(20 + i, gb.at[i], gp.at[i], partner)

    def first_x(j, yy):
        return rcopy(26 + 2 * j + yy, gp.at[j, 2 * yy + 1 - x], r1.at[j, yy], xn)

    def first_y(j, xx):
        return rcopy(32 + 2 * j + xx, gp.at[3 + j, 2 * (1 - y) + xx], r1.at[3 + j, xx], yn)

    def second_y(j):
        return rcopy(38 + j, p2.at[j, 1 - y], r2.at[j], yn)

    def second_x(j):
        return rcopy(41 + j, p2.at[3 + j, 1 - x], r2.at[3 + j], xn)

    def z_in(i):
        return rcopy(44 + i, rb.at[i], z1.at[i], zp)

    def z_mid(i):
        return rcopy(50 + i, zs.at[i], z2.at[i], zm)

    def z_out(i):
        return rcopy(56 + i, tt.at[k, i], tt.at[k, i], zp)

    def t_pair(i):
        return rcopy(87 + i, tt.at[k, i], tt.at[k, i], partner)

    for c in to_pair:
        c.start()
    for t in range(NT):
        for c in tok(t):
            c.start()

    def send_half(i, _):
        gload(i, 1 - k).wait()
        for q in range(4):
            gb[i, q] = gf[i, :, q * FC:(q + 1) * FC].astype(jnp.bfloat16)
        to_partner(i).start()
        gload(i, k).start()
        return 0

    lax.fori_loop(0, 6, send_half, 0)

    for m in range(3):
        local_shards[m].wait()
        to_pair[m].wait_recv()
        blk[0, m] = pair[0, m].T
    w_x.start()
    w_y.start()

    def own_tile(i):
        gload(i, k).wait()
        to_partner(i).wait_recv()
        for q in range(4):
            gp[i, q] = (gp[i, q].astype(jnp.float32)
                        + gf[i, :, q * FC:(q + 1) * FC].astype(jnp.bfloat16).astype(jnp.float32)).astype(jnp.bfloat16)

    def stage_a(j):
        own_tile(j)
        own_tile(3 + j)
        for b in range(2):
            first_x(j, b).start()
            first_y(j, b).start()

    def stage_b(j):
        for b in range(2):
            first_x(j, b).wait_recv()
            p2[j, b] = (gp[j, 2 * b + x].astype(jnp.float32) + r1[j, b].astype(jnp.float32)).astype(jnp.bfloat16)
            first_y(j, b).wait_recv()
            p2[3 + j, b] = (gp[3 + j, 2 * y + b].astype(jnp.float32)
                            + r1[3 + j, b].astype(jnp.float32)).astype(jnp.bfloat16)
        second_y(j).start()
        second_x(j).start()

    def second(i):
        return second_y(i) if i < 3 else second_x(i - 3)

    def mine(i):
        return y if i < 3 else x

    def stage_c(j):
        @pl.when(at_end)
        def _():
            for i in (j, 3 + j):
                second(i).wait_recv()
                rb[i] = (p2[i, mine(i)].astype(jnp.float32) + r2[i].astype(jnp.float32)).astype(jnp.bfloat16)
                z_in(i).start()

    def stage_d(i):
        @pl.when(inner)
        def _():
            second(i).wait_recv()
            z_in(i).wait_recv()
            zs[i] = (p2[i, mine(i)].astype(jnp.float32) + r2[i].astype(jnp.float32)) + z1[i].astype(jnp.float32)
            z_mid(i).start()

    def stage_e(i):
        @pl.when(inner)
        def _():
            z_mid(i).wait_recv()
            tt[k, i] = zs[i] + z2[i]
            z_out(i).start()
            t_pair(i).start()

    def v_start():
        for m in range(3):
            local_shards[3 + m].wait()
            to_pair[3 + m].wait_recv()
            vblk[m] = pair[1, m].T
            v_copies(m)[0].start()
            v_copies(m)[1].start()
        v_own.start()

    def w_1():
        w_x.wait_recv()
        w_zx.start()
        w_f1a.start()
        w_y.wait_recv()
        w_zy.start()
        w_f2a.start()

    def w_z():
        w_zy.wait_recv()
        w_f2b.start()

    def w_d():
        w_da.start()
        w_db.start()

    def w_3():
        w_da.wait_recv()
        w_db.wait_recv()
        w_f3.start()

    def v_1(m):
        v_x, v_y, v_f1, v_f2, v_da, v_db, _ = v_copies(m)
        v_x.wait_recv()
        v_da.start()
        v_f1.start()
        v_y.wait_recv()
        v_db.start()
        v_f2.start()

    def v_2(m):
        v_da, v_db, v_f3 = v_copies(m)[4:]
        v_da.wait_recv()
        v_db.wait_recv()
        v_f3.start()

    stages = {
        'A': stage_a, 'B': stage_b, 'C': stage_c,
        'D0': stage_d, 'D1': lambda j: stage_d(3 + j), 'E0': stage_e, 'E1': lambda j: stage_e(3 + j),
        'V': lambda j: v_start(), 'V1': v_1,
        'W1': lambda j: w_1(), 'WZ': lambda j: w_z(), 'WD': lambda j: w_d(), 'W3': lambda j: w_3(),
    }
    order = ('W1', 'WZ', 'W3', 'B', 'A', 'C', 'D0', 'D1', 'E0', 'E1', 'WD', 'V', 'V1')

    def tick(step):
        for name in order:
            for j, n in enumerate(STEPS[name]):
                if n < 24:
                    pl.when(step == n)(functools.partial(stages[name], j))

    def dw_out(c):
        cx, cy = c % 2, c // 2
        q = 2 * (y + cy - 2 * y * cy) + x + cx - 2 * x * cx
        return pltpu.make_async_copy(dwa, dw.at[:, :, pl.ds(pl.multiple_of(q * FC, FC), FC)], s_dw)

    def chunk(c, _):
        @pl.when(c == 1)
        def _():
            w_zx.wait_recv()
            w_f1b.start()
            w_f1a.wait_recv()
            w_f1b.wait_recv()

        @pl.when(c == 2)
        def _():
            w_f2a.wait_recv()
            w_f2b.wait_recv()

        @pl.when(c == 3)
        def _():
            w_f3.wait_recv()

        for m in range(3):
            wt[m * FC:(m + 1) * FC, :] = blk[c, m].T

        @pl.when(c > 0)
        def _():
            dw_out(c - 1).wait()

        dwa[...] = jnp.zeros_like(dwa)

        def tile(t, _):
            step = c * NT + t

            @pl.when(c == 0)
            def _():
                for cp in tok(t):
                    cp.wait()
                dxa[t] = jnp.zeros((D, T), jnp.float32)

            tick(step)
            xv = xs[t]
            yv = ys[t]
            a = dot(wt[0:FC, :], xv)
            b = dot(wt[FC:2 * FC, :], xv)
            dh = dot(wt[2 * FC:3 * FC, :], yv)
            sg = jnp.tanh(a * 0.5) * 0.5 + 0.5
            act = a * sg
            hb[...] = (act * b).astype(jnp.bfloat16)
            dab[FC:, :] = (dh * act).astype(jnp.bfloat16)
            dab[:FC, :] = (dh * b * (sg + act * (1.0 - sg))).astype(jnp.bfloat16)
            dxa[t] += dot(blk[c, 0], dab[:FC, :]) + dot(blk[c, 1], dab[FC:, :])
            gw = dot(xv, dab[...], NTD)
            dwa[0] += gw[:, :FC]
            dwa[1] += gw[:, FC:]
            dwa[2] += dot(yv, hb[...], NTD)
            return 0

        lax.fori_loop(0, NT, tile, 0)
        dw_out(c).start()
        return 0

    lax.fori_loop(0, 4, chunk, 0)

    def dx_out(t):
        return pltpu.make_async_copy(dxs.at[t % 2], dxt.at[:, pl.ds(pl.multiple_of(t * T, T), T)], s_dx.at[t % 2])

    def write_dx(t, _):
        @pl.when(t >= 2)
        def _():
            dx_out(t - 2).wait()

        dxs[t % 2] = dxa[t].astype(jnp.bfloat16)
        dx_out(t).start()
        return 0

    lax.fori_loop(0, NT, write_dx, 0)

    for name in order:
        for j, n in enumerate(STEPS[name]):
            if n >= 24:
                stages[name](j)

    for m in range(3):
        v_2(m)
    for i in (0, 3, 1, 4, 2, 5):
        @pl.when(at_end)
        def _():
            z_out(i).wait_recv()
            t_pair(i).start()
    for i in range(6):
        t_pair(i).wait_recv()

    def t_out(m):
        return pltpu.make_async_copy(to.at[m, pl.ds(pl.multiple_of(k * SH, SH), SH), :], gs.at[m], s_t.at[m])

    for m in range(3):
        to[m] = jnp.concatenate([tt[(4 * m + r) // 6, (4 * m + r) % 6] for r in range(4)], axis=0).T
        t_out(m).start()

    dw_out(3).wait()
    dx_out(NT - 2).wait()
    dx_out(NT - 1).wait()
    v_own.wait()
    for m in range(3):
        t_out(m).wait()
    for i in range(6):
        t_pair(i).wait_send()
        to_partner(i).wait_send()

        @pl.when(at_end)
        def _():
            z_in(i).wait_send()

        @pl.when(inner)
        def _():
            z_mid(i).wait_send()
            z_out(i).wait_send()
    for j in range(3):
        for b in range(2):
            first_x(j, b).wait_send()
            first_y(j, b).wait_send()
        second_x(j).wait_send()
        second_y(j).wait_send()
    for c in to_pair:
        c.wait_send()
    for c in (w_x, w_y, w_zx, w_zy, w_f1a, w_f1b, w_f2a, w_f2b, w_da, w_db, w_f3):
        c.wait_send()
    for m in range(3):
        for c in v_copies(m):
            c.wait_send()
        for c in (v_copies(m)[2], v_copies(m)[3], v_copies(m)[6]):
            c.wait_recv()


def step_kernel(xt, dyt, w1, w3, w2, v1, v3, v2, g):
    any_spec = pl.BlockSpec(memory_space=pl.ANY)
    bf, f32 = jnp.bfloat16, jnp.float32
    V = pltpu.VMEM
    dma = pltpu.SemaphoreType.DMA
    return pl.pallas_call(
        kernel,
        name='mlp_step',
        out_shape=(jax.ShapeDtypeStruct((D, N), bf), jax.ShapeDtypeStruct((3, D, F), f32),
                   jax.ShapeDtypeStruct((3, D, F), bf), jax.ShapeDtypeStruct((3, SH, D), f32)),
        in_specs=[any_spec] * 9,
        out_specs=(any_spec,) * 4,
        scratch_shapes=[
            V((NT, D, T), bf), V((NT, D, T), bf), V((2, 3, FC, D), bf), V((4, 3, D, FC), bf), V((3, D, FC), bf),
            V((3 * FC, D), bf), V((NT, D, T), f32), V((3, D, FC), f32), V((2 * FC, T), bf), V((FC, T), bf),
            V((2, D, T), bf),
            V((6, RT, F), f32), V((6, 4, RT, FC), bf), V((6, 4, RT, FC), bf), V((6, 2, RT, FC), bf),
            V((6, 2, RT, FC), bf), V((6, RT, FC), bf), V((6, RT, FC), bf), V((6, RT, FC), bf),
            V((6, RT, FC), f32), V((6, RT, FC), f32), V((2, 6, RT, FC), f32), V((3, FC, D), f32),
            dma((2, NT)), dma((6,)), dma((6,)), dma, dma((2,)), dma, dma((3,)), dma((93,)), dma((93,)),
        ],
        compiler_params=pltpu.CompilerParams(
            collective_id=0, has_side_effects=True, vmem_limit_bytes=67_000_000),
        cost_estimate=pl.CostEstimate(flops=43_500_000_000, bytes_accessed=60_000_000, transcendentals=4_718_592),
    )(xt, dyt, w1, w3, w2, v1, v3, v2, g)


def solution(mesh):
    def device_step(x_loc, dy_loc, w_gate, w_up, w_down, v_gate, v_up, v_down, g_next):
        dxt, dw, vo, gs = step_kernel(
            x_loc.T, dy_loc.T, w_gate.T, w_up.T, w_down, v_gate.T, v_up.T, v_down, g_next.reshape(3 * D, F))
        return dxt.T, gs.transpose(0, 2, 1), dw[None], vo[0], vo[1], vo[2].T

    row_spec = P(ALL_AXES, None)
    col_shard = P(None, FSDP_AXES)
    row_shard = P(FSDP_AXES, None)
    dev_spec = P(ALL_AXES, None, None, None)
    return jax.shard_map(
        device_step, mesh=mesh,
        in_specs=(row_spec, row_spec, col_shard, col_shard, row_shard, col_shard, col_shard, row_shard, dev_spec),
        out_specs=(row_spec, P(None, None, FSDP_AXES), dev_spec, P(), P(), P()),
        check_vma=False)
```

```python
import functools

import jax
import jax.numpy as jnp
from jax import lax
from jax.experimental import pallas as pl
from jax.experimental.pallas import tpu as pltpu
from jax.sharding import PartitionSpec as P

ALL_AXES = ('dp', 'col', 'fsdp')
FSDP_AXES = ('col', 'fsdp')
MESH = pl.DeviceIdType.MESH

D = 576
F = 1536
N = 3072
T = 512
NT = N // T
SH = 192
FC = 384
RT = 144
HR = D // 2
QR = HR // 2
NN = (((1,), (0,)), ((), ()))
NTD = (((1,), (1,)), ((), ()))

STEPS = {
    'A': (0, 1, 6), 'W1': (4,), 'WZ': (9,), 'WD': (12,), 'W3': (16,), 'V': (13,), 'V1': (20, 22, 24),
    'B': (6, 7, 10), 'C': (8, 11, 12),
    'D0': (10, 14, 17), 'D1': (12, 16, 19), 'E0': (14, 18, 22), 'E1': (16, 20, 24),
}


def dot(a, b, dn=NN):
    return lax.dot_general(a, b, dn, preferred_element_type=jnp.float32)


def kernel(xt, dyt, w1, w3, w2, v1, v3, v2, g, dxt, dw, vo, gs,
           xs, ys, pair, blk, vblk, wt, dxa, dwa, dab0, hb0, dab1, hb1,
           gf, gb, gp, r1, p2, r2, rb, z1, z2, zs, tt, to,
           s_tok, s_loc, s_g, s_dw, s_dx, s_vo, s_t, ss, rs):
    z = lax.axis_index('dp')
    y = lax.axis_index('col')
    f = lax.axis_index('fsdp')
    x = f // 2
    k = f % 2
    own = 2 * y + x
    partner = (z, y, f + 1 - 2 * k)
    xn = (z, y, (f + 2) % 4)
    yn = (z, 1 - y, f)
    z_pair = z + 1 - 2 * (z % 2)
    zp = (z_pair, y, f)
    zm = (3 - z, y, f)
    at_end = (z == 0) | (z == 3)
    inner = (z == 1) | (z == 2)

    def rcopy(n, src, dst, dev):
        return pltpu.make_async_remote_copy(
            src_ref=src, dst_ref=dst, send_sem=ss.at[n], recv_sem=rs.at[n], device_id=dev, device_id_type=MESH)

    def tok(t):
        cols = pl.ds(pl.multiple_of(t * T, T), T)
        return (pltpu.make_async_copy(xt.at[:, cols], xs.at[t], s_tok.at[0, t]),
                pltpu.make_async_copy(dyt.at[:, cols], ys.at[t], s_tok.at[1, t]))

    def gload(n):
        own_half = n >= 6
        o = n - 6
        i = jnp.where(own_half, (o % 2) * 3 + o // 2, n)
        h = jnp.where(own_half, k, 1 - k)
        r0 = pl.multiple_of(h * (6 * RT) + i * RT, RT)
        return pltpu.make_async_copy(g.at[pl.ds(r0, RT), :], gf.at[n % 4], s_g.at[n % 4])

    shards = ((w1, w3, w2), (v1, v3, v2))
    myrows = pl.ds(pl.multiple_of(k * SH, SH), SH)
    local_shards = [pltpu.make_async_copy(shards[u][m], pair.at[u, m, myrows, :], s_loc.at[3 * u + m])
                    for u in range(2) for m in range(3)]
    for n in range(4):
        gload(n).start()
    for c in local_shards:
        c.start()

    bar = pltpu.get_barrier_semaphore()
    for dev in (partner, xn, yn, zp, zm):
        pl.semaphore_signal(bar, inc=1, device_id=dev, device_id_type=MESH)
    pl.semaphore_wait(bar, 5)

    to_pair = [rcopy(3 * u + m, shards[u][m], pair.at[u, m, myrows, :], partner) for u in range(2) for m in range(3)]
    half = pl.ds(pl.multiple_of(k * HR, HR), HR)
    other = pl.ds(pl.multiple_of((1 - k) * HR, HR), HR)
    qa = pl.ds(pl.multiple_of(k * HR, QR), QR)
    qb = pl.ds(pl.multiple_of(k * HR + QR, QR), QR)

    def blkcols(cx, cy):
        xx = 1 - x if cx else x
        yy = 1 - y if cy else y
        return pl.ds(pl.multiple_of((2 * yy + xx) * FC, FC), FC)

    zo = z % 2
    qm = pl.ds(pl.multiple_of(k * HR + zo * QR, QR), QR)
    qo = pl.ds(pl.multiple_of(k * HR + (1 - zo) * QR, QR), QR)
    w_x = rcopy(6, blk.at[0, qm, :], blk.at[1, qm, :], xn)
    w_y = rcopy(7, blk.at[0, qm, :], blk.at[2, qm, :], yn)
    w_zx = rcopy(8, blk.at[1, qm, :], blk.at[1, qm, :], zp)
    w_zy = rcopy(9, blk.at[2, qm, :], blk.at[2, qm, :], zp)
    w_f1a = rcopy(62, blk.at[1, qm, :], blk.at[1, qm, :], partner)
    w_f1b = rcopy(63, blk.at[1, qo, :], blk.at[1, qo, :], partner)
    w_f2a = rcopy(64, blk.at[2, qm, :], blk.at[2, qm, :], partner)
    w_f2b = rcopy(65, blk.at[2, qo, :], blk.at[2, qo, :], partner)
    w_da = rcopy(10, blk.at[1, qa, :], blk.at[3, qa, :], yn)
    w_db = rcopy(11, blk.at[2, qb, :], blk.at[3, qb, :], xn)
    w_f3 = rcopy(12, blk.at[3, half, :], blk.at[3, half, :], partner)

    v_own = pltpu.make_async_copy(vblk, vo.at[:, :, blkcols(0, 0)], s_vo)
    def v_copies(m):
        n = 66 + 7 * m
        q0, q1, q2, q3 = blkcols(0, 0), blkcols(1, 0), blkcols(0, 1), blkcols(1, 1)
        return (rcopy(n, vblk.at[m, half, :], vo.at[m, half, q0], xn),
                rcopy(n + 1, vblk.at[m, half, :], vo.at[m, half, q0], yn),
                rcopy(n + 2, vo.at[m, half, q1], vo.at[m, half, q1], partner),
                rcopy(n + 3, vo.at[m, half, q2], vo.at[m, half, q2], partner),
                rcopy(n + 4, vo.at[m, qa, q1], vo.at[m, qa, q1], yn),
                rcopy(n + 5, vo.at[m, qb, q2], vo.at[m, qb, q2], xn),
                rcopy(n + 6, vo.at[m, half, q3], vo.at[m, half, q3], partner))

    def to_partner(i):
        return rcopy(20 + i, gb.at[i], gp.at[i], partner)

    def first_x(j, yy):
        return rcopy(26 + 2 * j + yy, gp.at[j, 2 * yy + 1 - x], r1.at[j, yy], xn)

    def first_y(j, xx):
        return rcopy(32 + 2 * j + xx, gp.at[3 + j, 2 * (1 - y) + xx], r1.at[3 + j, xx], yn)

    def second_y(j):
        return rcopy(38 + j, p2.at[j, 1 - y], r2.at[j], yn)

    def second_x(j):
        return rcopy(41 + j, p2.at[3 + j, 1 - x], r2.at[3 + j], xn)

    def z_in(i):
        return rcopy(44 + i, rb.at[i], z1.at[i], zp)

    def z_mid(i):
        return rcopy(50 + i, zs.at[i], z2.at[i], zm)

    def z_out(i):
        return rcopy(56 + i, tt.at[k, i], tt.at[k, i], zp)

    def t_pair(i):
        return rcopy(87 + i, tt.at[k, i], tt.at[k, i], partner)

    for c in to_pair:
        c.start()
    for t in range(NT):
        for c in tok(t):
            c.start()

    def send_half(i, _):
        gload(i).wait()
        for q in range(4):
            gb[i, q] = gf[i % 4, :, q * FC:(q + 1) * FC].astype(jnp.bfloat16)
        to_partner(i).start()
        gload(i + 4).start()
        return 0

    lax.fori_loop(0, 6, send_half, 0)

    for m in range(3):
        local_shards[m].wait()
        to_pair[m].wait_recv()
        blk[0, :, m * FC:(m + 1) * FC] = pair[0, m].T
    w_x.start()
    w_y.start()

    def own_tile(n, i):
        gload(n).wait()
        to_partner(i).wait_recv()
        for q in range(4):
            gp[i, q] = (gp[i, q].astype(jnp.float32)
                        + gf[n % 4, :, q * FC:(q + 1) * FC].astype(jnp.bfloat16).astype(jnp.float32)
                        ).astype(jnp.bfloat16)
        if n + 4 < 12:
            gload(n + 4).start()

    def stage_a(j):
        own_tile(6 + 2 * j, j)
        own_tile(7 + 2 * j, 3 + j)
        for b in range(2):
            first_x(j, b).start()
            first_y(j, b).start()

    def stage_b(j):
        for b in range(2):
            first_x(j, b).wait_recv()
            p2[j, b] = (gp[j, 2 * b + x].astype(jnp.float32) + r1[j, b].astype(jnp.float32)).astype(jnp.bfloat16)
            first_y(j, b).wait_recv()
            p2[3 + j, b] = (gp[3 + j, 2 * y + b].astype(jnp.float32)
                            + r1[3 + j, b].astype(jnp.float32)).astype(jnp.bfloat16)
        second_y(j).start()
        second_x(j).start()

    def second(i):
        return second_y(i) if i < 3 else second_x(i - 3)

    def mine(i):
        return y if i < 3 else x

    def stage_c(j):
        @pl.when(at_end)
        def _():
            for i in (j, 3 + j):
                second(i).wait_recv()
                rb[i] = (p2[i, mine(i)].astype(jnp.float32) + r2[i].astype(jnp.float32)).astype(jnp.bfloat16)
                z_in(i).start()

    def stage_d(i):
        @pl.when(inner)
        def _():
            second(i).wait_recv()
            z_in(i).wait_recv()
            zs[i] = (p2[i, mine(i)].astype(jnp.float32) + r2[i].astype(jnp.float32)) + z1[i].astype(jnp.float32)
            z_mid(i).start()

    def stage_e(i):
        @pl.when(inner)
        def _():
            z_mid(i).wait_recv()
            tt[k, i] = zs[i] + z2[i]
            z_out(i).start()
            t_pair(i).start()

    def v_start():
        for m in range(3):
            local_shards[3 + m].wait()
            to_pair[3 + m].wait_recv()
            vblk[m] = pair[1, m].T
            v_copies(m)[0].start()
            v_copies(m)[1].start()
        v_own.start()

    def w_1():
        w_x.wait_recv()
        w_zx.start()
        w_f1a.start()
        w_y.wait_recv()
        w_zy.start()
        w_f2a.start()

    def w_z():
        w_zy.wait_recv()
        w_f2b.start()

    def w_d():
        w_da.start()
        w_db.start()

    def w_3():
        w_da.wait_recv()
        w_db.wait_recv()
        w_f3.start()

    def v_1(m):
        v_x, v_y, v_f1, v_f2, v_da, v_db, _ = v_copies(m)
        v_x.wait_recv()
        v_da.start()
        v_f1.start()
        v_y.wait_recv()
        v_db.start()
        v_f2.start()

    def v_2(m):
        v_da, v_db, v_f3 = v_copies(m)[4:]
        v_da.wait_recv()
        v_db.wait_recv()
        v_f3.start()

    stages = {
        'A': stage_a, 'B': stage_b, 'C': stage_c,
        'D0': stage_d, 'D1': lambda j: stage_d(3 + j), 'E0': stage_e, 'E1': lambda j: stage_e(3 + j),
        'V': lambda j: v_start(), 'V1': v_1,
        'W1': lambda j: w_1(), 'WZ': lambda j: w_z(), 'WD': lambda j: w_d(), 'W3': lambda j: w_3(),
    }
    order = ('W1', 'WZ', 'W3', 'B', 'A', 'C', 'D0', 'D1', 'E0', 'E1', 'WD', 'V', 'V1')

    def tick(step, steps):
        for name in order:
            for j, n in enumerate(STEPS[name]):
                if n in steps:
                    if len(steps) == 1:
                        stages[name](j)
                    else:
                        pl.when(step == n)(functools.partial(stages[name], j))

    def dw_out(c):
        cx, cy = c % 2, c // 2
        q = 2 * (y + cy - 2 * y * cy) + x + cx - 2 * x * cx
        return pltpu.make_async_copy(
            dwa.at[c % 2], dw.at[:, :, pl.ds(pl.multiple_of(q * FC, FC), FC)], s_dw.at[c % 2])

    def head(c):
        @pl.when(c == 1)
        def _():
            w_zx.wait_recv()
            w_f1b.start()
            w_f1a.wait_recv()
            w_f1b.wait_recv()

        @pl.when(c == 2)
        def _():
            w_f2a.wait_recv()
            w_f2b.wait_recv()

        @pl.when(c == 3)
        def _():
            w_f3.wait_recv()

        for m in range(3):
            wt[m * FC:(m + 1) * FC, :] = blk[c, :, m * FC:(m + 1) * FC].T

        @pl.when(c >= 2)
        def _():
            dw_out(c - 2).wait()

        dwa[c % 2] = jnp.zeros((3, D, FC), jnp.float32)

    def first_touch(t):
        for cp in tok(t):
            cp.wait()
        dxa[t] = jnp.zeros((D, T), jnp.float32)

    def forward(t, dab, hb):
        xv = xs[t]
        a = dot(wt[0:FC, :], xv)
        b = dot(wt[FC:2 * FC, :], xv)
        dh = dot(wt[2 * FC:3 * FC, :], ys[t])
        sg = jnp.tanh(a * 0.5) * 0.5 + 0.5
        act = a * sg
        hb[...] = (act * b).astype(jnp.bfloat16)
        dab[FC:, :] = (dh * act).astype(jnp.bfloat16)
        dab[:FC, :] = (dh * b * (sg + act * (1.0 - sg))).astype(jnp.bfloat16)

    def backward(step, dab, hb):
        c, t = step // NT, step % NT
        dxa[t] += dot(blk[c, :, :2 * FC], dab[...])
        gw = dot(xs[t], dab[...], NTD)
        dwa[c % 2, 0] += gw[:, :FC]
        dwa[c % 2, 1] += gw[:, FC:]
        dwa[c % 2, 2] += dot(ys[t], hb[...], NTD)

    def half_step(step, steps, src, dst):
        c, t = step // NT, step % NT
        if any(n % NT == 0 for n in steps):
            @pl.when(t == 0)
            def _():
                head(c)

        if any(n % NT == 1 and n > NT for n in steps):
            @pl.when((t == 1) & (c > 0))
            def _():
                dw_out(c - 1).start()

        if any(n < NT for n in steps):
            @pl.when(c == 0)
            def _():
                first_touch(t)

        tick(step, steps)
        forward(t, *dst)
        backward(step - 1, *src)

    b0, b1 = (dab0, hb0), (dab1, hb1)
    head(0)
    first_touch(0)
    tick(0, (0,))
    forward(0, *b0)

    def two_steps(p, _):
        half_step(2 * p + 1, tuple(range(1, 23, 2)), b0, b1)
        half_step(2 * p + 2, tuple(range(2, 23, 2)), b1, b0)
        return 0

    lax.fori_loop(0, 11, two_steps, 0)
    half_step(23, (23,), b0, b1)
    backward(23, *b1)
    dw_out(3).start()

    def dx_out(t):
        return pltpu.make_async_copy(xs.at[t], dxt.at[:, pl.ds(pl.multiple_of(t * T, T), T)], s_dx.at[t])

    def write_dx(t, _):
        xs[t] = dxa[t].astype(jnp.bfloat16)
        dx_out(t).start()
        return 0

    lax.fori_loop(0, NT, write_dx, 0)

    for name in order:
        for j, n in enumerate(STEPS[name]):
            if n >= 24:
                stages[name](j)

    for m in range(3):
        v_2(m)
    for i in (0, 3, 1, 4, 2, 5):
        @pl.when(at_end)
        def _():
            z_out(i).wait_recv()
            t_pair(i).start()
    for i in range(6):
        t_pair(i).wait_recv()

    def t_out(m):
        return pltpu.make_async_copy(to.at[m], gs.at[m], s_t.at[m])

    for m in range(3):
        full = jnp.concatenate([tt[(4 * m + r) // 6, (4 * m + r) % 6] for r in range(4)], axis=0).T

        @pl.when(k == 0)
        def _():
            to[m] = full[:SH]

        @pl.when(k == 1)
        def _():
            to[m] = full[SH:]

        t_out(m).start()

    dw_out(2).wait()
    dw_out(3).wait()
    for t in range(NT):
        dx_out(t).wait()
    v_own.wait()
    for m in range(3):
        t_out(m).wait()
    for i in range(6):
        t_pair(i).wait_send()
        to_partner(i).wait_send()

        @pl.when(at_end)
        def _():
            z_in(i).wait_send()

        @pl.when(inner)
        def _():
            z_mid(i).wait_send()
            z_out(i).wait_send()
    for j in range(3):
        for b in range(2):
            first_x(j, b).wait_send()
            first_y(j, b).wait_send()
        second_x(j).wait_send()
        second_y(j).wait_send()
    for c in to_pair:
        c.wait_send()
    for c in (w_x, w_y, w_zx, w_zy, w_f1a, w_f1b, w_f2a, w_f2b, w_da, w_db, w_f3):
        c.wait_send()
    for m in range(3):
        for c in v_copies(m):
            c.wait_send()
        for c in (v_copies(m)[2], v_copies(m)[3], v_copies(m)[6]):
            c.wait_recv()


def step_kernel(xt, dyt, w1, w3, w2, v1, v3, v2, g):
    any_spec = pl.BlockSpec(memory_space=pl.ANY)
    bf, f32 = jnp.bfloat16, jnp.float32
    V = pltpu.VMEM
    dma = pltpu.SemaphoreType.DMA
    return pl.pallas_call(
        kernel,
        name='mlp_step',
        out_shape=(jax.ShapeDtypeStruct((D, N), bf), jax.ShapeDtypeStruct((3, D, F), f32),
                   jax.ShapeDtypeStruct((3, D, F), bf), jax.ShapeDtypeStruct((3, SH, D), f32)),
        in_specs=[any_spec] * 9,
        out_specs=(any_spec,) * 4,
        scratch_shapes=[
            V((NT, D, T), bf), V((NT, D, T), bf), V((2, 3, FC, D), bf), V((4, D, 3 * FC), bf), V((3, D, FC), bf),
            V((3 * FC, D), bf), V((NT, D, T), f32), V((2, 3, D, FC), f32),
            V((2 * FC, T), bf), V((FC, T), bf), V((2 * FC, T), bf), V((FC, T), bf),
            V((4, RT, F), f32), V((6, 4, RT, FC), bf), V((6, 4, RT, FC), bf), V((6, 2, RT, FC), bf),
            V((6, 2, RT, FC), bf), V((6, RT, FC), bf), V((6, RT, FC), bf), V((6, RT, FC), bf),
            V((6, RT, FC), f32), V((6, RT, FC), f32), V((2, 6, RT, FC), f32), V((3, SH, D), f32),
            dma((2, NT)), dma((6,)), dma((4,)), dma((2,)), dma((NT,)), dma, dma((3,)), dma((93,)), dma((93,)),
        ],
        compiler_params=pltpu.CompilerParams(
            collective_id=0, has_side_effects=True, vmem_limit_bytes=67_000_000),
        cost_estimate=pl.CostEstimate(flops=43_500_000_000, bytes_accessed=60_000_000, transcendentals=4_718_592),
    )(xt, dyt, w1, w3, w2, v1, v3, v2, g)


def solution(mesh):
    def device_step(x_loc, dy_loc, w_gate, w_up, w_down, v_gate, v_up, v_down, g_next):
        dxt, dw, vo, gs = step_kernel(
            x_loc.T, dy_loc.T, w_gate.T, w_up.T, w_down, v_gate.T, v_up.T, v_down, g_next.reshape(3 * D, F))
        return dxt.T, gs.transpose(0, 2, 1), dw[None], vo[0], vo[1], vo[2].T

    row_spec = P(ALL_AXES, None)
    col_shard = P(None, FSDP_AXES)
    row_shard = P(FSDP_AXES, None)
    dev_spec = P(ALL_AXES, None, None, None)
    return jax.shard_map(
        device_step, mesh=mesh,
        in_specs=(row_spec, row_spec, col_shard, col_shard, row_shard, col_shard, col_shard, row_shard, dev_spec),
        out_specs=(row_spec, P(None, None, FSDP_AXES), dev_spec, P(), P(), P()),
        check_vma=False)
```

```python
import functools

import jax
import jax.numpy as jnp
from jax import lax
from jax.experimental import pallas as pl
from jax.experimental.pallas import tpu as pltpu
from jax.sharding import PartitionSpec as P

ALL_AXES = ('dp', 'col', 'fsdp')
FSDP_AXES = ('col', 'fsdp')
MESH = pl.DeviceIdType.MESH

D = 576
F = 1536
N = 3072
T = 512
NT = N // T
SH = 192
FC = 384
RT = 144
HR = D // 2
QR = HR // 2
NN = (((1,), (0,)), ((), ()))
NTD = (((1,), (1,)), ((), ()))

STEPS = {
    'AX': (0, 5, 7), 'AY': (0, 1, 2), 'BX': (7, 10, 13), 'BY': (5, 6, 8), 'CX': (9, 13, 15), 'CY': (8, 11, 14),
    'W1': (3,), 'WZ': (6,), 'WDA': (7,), 'WDB': (9,), 'W3': (16,), 'V': (13,), 'V1': (18, 20, 22),
    'D0': (11, 15, 17), 'D1': (10, 13, 16), 'E0': (15, 19, 22), 'E1': (13, 17, 20),
}


def dot(a, b, dn=NN):
    return lax.dot_general(a, b, dn, preferred_element_type=jnp.float32)


def kernel(xt, dyt, w1, w3, w2, v1, v3, v2, g, dxt, dw, vo, gs,
           xs, ys, pair, blk, vblk, wt, dxa, dwa, dab0, hb0, dab1, hb1,
           gf, gb, gp, r1, p2, r2, rb, z1, z2, zs, tt, to,
           s_tok, s_loc, s_g, s_dw, s_dx, s_vo, s_t, ss, rs):
    z = lax.axis_index('dp')
    y = lax.axis_index('col')
    f = lax.axis_index('fsdp')
    x = f // 2
    k = f % 2
    own = 2 * y + x
    partner = (z, y, f + 1 - 2 * k)
    xn = (z, y, (f + 2) % 4)
    yn = (z, 1 - y, f)
    z_pair = z + 1 - 2 * (z % 2)
    zp = (z_pair, y, f)
    zm = (3 - z, y, f)
    at_end = (z == 0) | (z == 3)
    inner = (z == 1) | (z == 2)

    def rcopy(n, src, dst, dev):
        return pltpu.make_async_remote_copy(
            src_ref=src, dst_ref=dst, send_sem=ss.at[n], recv_sem=rs.at[n], device_id=dev, device_id_type=MESH)

    def tok(t):
        cols = pl.ds(pl.multiple_of(t * T, T), T)
        return (pltpu.make_async_copy(xt.at[:, cols], xs.at[t], s_tok.at[0, t]),
                pltpu.make_async_copy(dyt.at[:, cols], ys.at[t], s_tok.at[1, t]))

    def g_tile(o):
        return jnp.where(o == 0, 0, jnp.where(o < 4, o + 2, o - 3))

    def gload(n):
        own_half = n >= 6
        o = jnp.where(own_half, n - 6, n)
        i = g_tile(o)
        h = jnp.where(own_half, k, 1 - k)
        r0 = pl.multiple_of(h * (6 * RT) + i * RT, RT)
        return pltpu.make_async_copy(g.at[pl.ds(r0, RT), :], gf.at[n % 4], s_g.at[n % 4])

    shards = ((w1, w3, w2), (v1, v3, v2))
    myrows = pl.ds(pl.multiple_of(k * SH, SH), SH)
    local_shards = [pltpu.make_async_copy(shards[u][m], pair.at[u, m, myrows, :], s_loc.at[3 * u + m])
                    for u in range(2) for m in range(3)]
    for n in range(4):
        gload(n).start()
    for c in local_shards:
        c.start()

    bar = pltpu.get_barrier_semaphore()
    for dev in (partner, xn, yn, zp, zm):
        pl.semaphore_signal(bar, inc=1, device_id=dev, device_id_type=MESH)
    pl.semaphore_wait(bar, 5)

    to_pair = [rcopy(3 * u + m, shards[u][m], pair.at[u, m, myrows, :], partner) for u in range(2) for m in range(3)]
    half = pl.ds(pl.multiple_of(k * HR, HR), HR)
    other = pl.ds(pl.multiple_of((1 - k) * HR, HR), HR)
    qa = pl.ds(pl.multiple_of(k * HR, QR), QR)
    qb = pl.ds(pl.multiple_of(k * HR + QR, QR), QR)

    def blkcols(cx, cy):
        xx = 1 - x if cx else x
        yy = 1 - y if cy else y
        return pl.ds(pl.multiple_of((2 * yy + xx) * FC, FC), FC)

    zo = z % 2
    qm = pl.ds(pl.multiple_of(k * HR + zo * QR, QR), QR)
    qo = pl.ds(pl.multiple_of(k * HR + (1 - zo) * QR, QR), QR)
    w_x = rcopy(6, blk.at[0, half, :], blk.at[1, half, :], xn)
    w_y = rcopy(7, blk.at[0, qm, :], blk.at[2, qm, :], yn)
    w_zy = rcopy(9, blk.at[2, qm, :], blk.at[2, qm, :], zp)
    w_f1 = rcopy(62, blk.at[1, half, :], blk.at[1, half, :], partner)
    w_f2a = rcopy(64, blk.at[2, qm, :], blk.at[2, qm, :], partner)
    w_f2b = rcopy(65, blk.at[2, qo, :], blk.at[2, qo, :], partner)
    w_da = rcopy(10, blk.at[1, qa, :], blk.at[3, qa, :], yn)
    w_db = rcopy(11, blk.at[2, qb, :], blk.at[3, qb, :], xn)
    w_f3 = rcopy(12, blk.at[3, half, :], blk.at[3, half, :], partner)

    v_own = pltpu.make_async_copy(vblk, vo.at[:, :, blkcols(0, 0)], s_vo)
    def v_copies(m):
        n = 66 + 7 * m
        q0, q1, q2, q3 = blkcols(0, 0), blkcols(1, 0), blkcols(0, 1), blkcols(1, 1)
        return (rcopy(n, vblk.at[m, half, :], vo.at[m, half, q0], xn),
                rcopy(n + 1, vblk.at[m, half, :], vo.at[m, half, q0], yn),
                rcopy(n + 2, vo.at[m, half, q1], vo.at[m, half, q1], partner),
                rcopy(n + 3, vo.at[m, half, q2], vo.at[m, half, q2], partner),
                rcopy(n + 4, vo.at[m, qa, q1], vo.at[m, qa, q1], yn),
                rcopy(n + 5, vo.at[m, qb, q2], vo.at[m, qb, q2], xn),
                rcopy(n + 6, vo.at[m, half, q3], vo.at[m, half, q3], partner))

    def to_partner(i):
        return rcopy(20 + i, gb.at[i], gp.at[i], partner)

    def first_x(j, yy):
        return rcopy(26 + 2 * j + yy, gp.at[j, 2 * yy + 1 - x], r1.at[j, yy], xn)

    def first_y(j, xx):
        return rcopy(32 + 2 * j + xx, gp.at[3 + j, 2 * (1 - y) + xx], r1.at[3 + j, xx], yn)

    def second_y(j):
        return rcopy(38 + j, p2.at[j, 1 - y], r2.at[j], yn)

    def second_x(j):
        return rcopy(41 + j, p2.at[3 + j, 1 - x], r2.at[3 + j], xn)

    def z_in(i):
        return rcopy(44 + i, rb.at[i], z1.at[i], zp)

    def z_mid(i):
        return rcopy(50 + i, zs.at[i], z2.at[i], zm)

    def z_out(i):
        return rcopy(56 + i, tt.at[k, i], tt.at[k, i], zp)

    def t_pair(i):
        return rcopy(87 + i, tt.at[k, i], tt.at[k, i], partner)

    for c in to_pair:
        c.start()
    for t in range(NT):
        for c in tok(t):
            c.start()

    def send_half(n, _):
        i = g_tile(n)
        gload(n).wait()
        for q in range(4):
            gb[i, q] = gf[n % 4, :, q * FC:(q + 1) * FC].astype(jnp.bfloat16)
        to_partner(i).start()
        gload(n + 4).start()
        return 0

    lax.fori_loop(0, 2, send_half, 0)

    for m in range(3):
        local_shards[m].wait()
        to_pair[m].wait_recv()
        blk[0, :, m * FC:(m + 1) * FC] = pair[0, m].T
    w_x.start()
    w_y.start()
    lax.fori_loop(2, 6, send_half, 0)

    def own_tile(i):
        n = 6 + (0, 4, 5, 1, 2, 3)[i]
        gload(n).wait()
        to_partner(i).wait_recv()
        for q in range(4):
            gp[i, q] = (gp[i, q].astype(jnp.float32)
                        + gf[n % 4, :, q * FC:(q + 1) * FC].astype(jnp.bfloat16).astype(jnp.float32)
                        ).astype(jnp.bfloat16)
        if n + 4 < 12:
            gload(n + 4).start()

    def stage_ax(j):
        own_tile(j)
        for b in range(2):
            first_x(j, b).start()

    def stage_ay(j):
        own_tile(3 + j)
        for b in range(2):
            first_y(j, b).start()

    def stage_bx(j):
        for b in range(2):
            first_x(j, b).wait_recv()
            p2[j, b] = (gp[j, 2 * b + x].astype(jnp.float32) + r1[j, b].astype(jnp.float32)).astype(jnp.bfloat16)
        second_y(j).start()

    def stage_by(j):
        for b in range(2):
            first_y(j, b).wait_recv()
            p2[3 + j, b] = (gp[3 + j, 2 * y + b].astype(jnp.float32)
                            + r1[3 + j, b].astype(jnp.float32)).astype(jnp.bfloat16)
        second_x(j).start()

    def second(i):
        return second_y(i) if i < 3 else second_x(i - 3)

    def mine(i):
        return y if i < 3 else x

    def stage_c(i):
        @pl.when(at_end)
        def _():
            second(i).wait_recv()
            rb[i] = (p2[i, mine(i)].astype(jnp.float32) + r2[i].astype(jnp.float32)).astype(jnp.bfloat16)
            z_in(i).start()

    def stage_d(i):
        @pl.when(inner)
        def _():
            second(i).wait_recv()
            z_in(i).wait_recv()
            zs[i] = (p2[i, mine(i)].astype(jnp.float32) + r2[i].astype(jnp.float32)) + z1[i].astype(jnp.float32)
            z_mid(i).start()

    def stage_e(i):
        @pl.when(inner)
        def _():
            z_mid(i).wait_recv()
            tt[k, i] = zs[i] + z2[i]
            z_out(i).start()
            t_pair(i).start()

    def v_start():
        for m in range(3):
            local_shards[3 + m].wait()
            to_pair[3 + m].wait_recv()
            vblk[m] = pair[1, m].T
            v_copies(m)[0].start()
            v_copies(m)[1].start()
        v_own.start()

    def w_1():
        w_y.wait_recv()
        w_zy.start()
        w_f2a.start()

    def w_z():
        w_zy.wait_recv()
        w_f2b.start()

    def w_3():
        w_da.wait_recv()
        w_db.wait_recv()
        w_f3.start()

    def v_1(m):
        v_x, v_y, v_f1, v_f2, v_da, v_db, _ = v_copies(m)
        v_x.wait_recv()
        v_da.start()
        v_f1.start()
        v_y.wait_recv()
        v_db.start()
        v_f2.start()

    def v_2(m):
        v_da, v_db, v_f3 = v_copies(m)[4:]
        v_da.wait_recv()
        v_db.wait_recv()
        v_f3.start()

    stages = {
        'AX': stage_ax, 'AY': stage_ay, 'BX': stage_bx, 'BY': stage_by,
        'CX': stage_c, 'CY': lambda j: stage_c(3 + j),
        'D0': stage_d, 'D1': lambda j: stage_d(3 + j), 'E0': stage_e, 'E1': lambda j: stage_e(3 + j),
        'V': lambda j: v_start(), 'V1': v_1,
        'W1': lambda j: w_1(), 'WZ': lambda j: w_z(), 'WDA': lambda j: w_da.start(), 'WDB': lambda j: w_db.start(),
        'W3': lambda j: w_3(),
    }
    order = ('W1', 'WZ', 'W3', 'BX', 'BY', 'AX', 'AY', 'CX', 'CY', 'D0', 'D1', 'E0', 'E1', 'WDA', 'WDB', 'V', 'V1')

    def tick(step, steps):
        for name in order:
            for j, n in enumerate(STEPS[name]):
                if n in steps:
                    if len(steps) == 1:
                        stages[name](j)
                    else:
                        pl.when(step == n)(functools.partial(stages[name], j))

    def dw_out(c):
        cx, cy = c % 2, c // 2
        q = 2 * (y + cy - 2 * y * cy) + x + cx - 2 * x * cx
        return pltpu.make_async_copy(
            dwa.at[c % 2], dw.at[:, :, pl.ds(pl.multiple_of(q * FC, FC), FC)], s_dw.at[c % 2])

    def head(c):
        @pl.when(c == 1)
        def _():
            w_x.wait_recv()
            w_f1.start()
            w_f1.wait_recv()

        @pl.when(c == 2)
        def _():
            w_f2a.wait_recv()
            w_f2b.wait_recv()

        @pl.when(c == 3)
        def _():
            w_f3.wait_recv()

        for m in range(3):
            wt[m * FC:(m + 1) * FC, :] = blk[c, :, m * FC:(m + 1) * FC].T

        @pl.when(c >= 2)
        def _():
            dw_out(c - 2).wait()

        dwa[c % 2] = jnp.zeros((3, D, FC), jnp.float32)

    def first_touch(t):
        for cp in tok(t):
            cp.wait()
        dxa[t] = jnp.zeros((D, T), jnp.float32)

    def forward(t, dab, hb):
        xv = xs[t]
        a = dot(wt[0:FC, :], xv)
        b = dot(wt[FC:2 * FC, :], xv)
        dh = dot(wt[2 * FC:3 * FC, :], ys[t])
        sg = jnp.tanh(a * 0.5) * 0.5 + 0.5
        act = a * sg
        hb[...] = (act * b).astype(jnp.bfloat16)
        dab[FC:, :] = (dh * act).astype(jnp.bfloat16)
        dab[:FC, :] = (dh * b * (sg + act * (1.0 - sg))).astype(jnp.bfloat16)

    def backward(step, dab, hb):
        c, t = step // NT, step % NT
        dxa[t] += dot(blk[c, :, :2 * FC], dab[...])
        gw = dot(xs[t], dab[...], NTD)
        dwa[c % 2, 0] += gw[:, :FC]
        dwa[c % 2, 1] += gw[:, FC:]
        dwa[c % 2, 2] += dot(ys[t], hb[...], NTD)

    def half_step(step, steps, src, dst):
        c, t = step // NT, step % NT
        if any(n % NT == 0 for n in steps):
            @pl.when(t == 0)
            def _():
                head(c)

        if any(n % NT == 1 and n > NT for n in steps):
            @pl.when((t == 1) & (c > 0))
            def _():
                dw_out(c - 1).start()

        if any(n < NT for n in steps):
            @pl.when(c == 0)
            def _():
                first_touch(t)

        tick(step, steps)
        forward(t, *dst)
        backward(step - 1, *src)

    b0, b1 = (dab0, hb0), (dab1, hb1)
    head(0)
    first_touch(0)
    tick(0, (0,))
    forward(0, *b0)

    def two_steps(p, _):
        half_step(2 * p + 1, tuple(range(1, 23, 2)), b0, b1)
        half_step(2 * p + 2, tuple(range(2, 23, 2)), b1, b0)
        return 0

    lax.fori_loop(0, 11, two_steps, 0)
    half_step(23, (23,), b0, b1)
    backward(23, *b1)
    dw_out(3).start()

    def dx_out(t):
        return pltpu.make_async_copy(xs.at[t], dxt.at[:, pl.ds(pl.multiple_of(t * T, T), T)], s_dx.at[t])

    def write_dx(t, _):
        xs[t] = dxa[t].astype(jnp.bfloat16)
        dx_out(t).start()
        return 0

    lax.fori_loop(0, NT, write_dx, 0)

    for name in order:
        for j, n in enumerate(STEPS[name]):
            if n >= 24:
                stages[name](j)

    for m in range(3):
        v_2(m)
    for i in (0, 3, 1, 4, 2, 5):
        @pl.when(at_end)
        def _():
            z_out(i).wait_recv()
            t_pair(i).start()
    for i in range(6):
        t_pair(i).wait_recv()

    def t_out(m):
        return pltpu.make_async_copy(to.at[m], gs.at[m], s_t.at[m])

    for m in range(3):
        full = jnp.concatenate([tt[(4 * m + r) // 6, (4 * m + r) % 6] for r in range(4)], axis=0).T

        @pl.when(k == 0)
        def _():
            to[m] = full[:SH]

        @pl.when(k == 1)
        def _():
            to[m] = full[SH:]

        t_out(m).start()

    dw_out(2).wait()
    dw_out(3).wait()
    for t in range(NT):
        dx_out(t).wait()
    v_own.wait()
    for m in range(3):
        t_out(m).wait()
    for i in range(6):
        t_pair(i).wait_send()
        to_partner(i).wait_send()

        @pl.when(at_end)
        def _():
            z_in(i).wait_send()

        @pl.when(inner)
        def _():
            z_mid(i).wait_send()
            z_out(i).wait_send()
    for j in range(3):
        for b in range(2):
            first_x(j, b).wait_send()
            first_y(j, b).wait_send()
        second_x(j).wait_send()
        second_y(j).wait_send()
    for c in to_pair:
        c.wait_send()
    for c in (w_x, w_y, w_zy, w_f1, w_f2a, w_f2b, w_da, w_db, w_f3):
        c.wait_send()
    for m in range(3):
        for c in v_copies(m):
            c.wait_send()
        for c in (v_copies(m)[2], v_copies(m)[3], v_copies(m)[6]):
            c.wait_recv()


def step_kernel(xt, dyt, w1, w3, w2, v1, v3, v2, g):
    any_spec = pl.BlockSpec(memory_space=pl.ANY)
    bf, f32 = jnp.bfloat16, jnp.float32
    V = pltpu.VMEM
    dma = pltpu.SemaphoreType.DMA
    return pl.pallas_call(
        kernel,
        name='mlp_step',
        out_shape=(jax.ShapeDtypeStruct((D, N), bf), jax.ShapeDtypeStruct((3, D, F), f32),
                   jax.ShapeDtypeStruct((3, D, F), bf), jax.ShapeDtypeStruct((3, SH, D), f32)),
        in_specs=[any_spec] * 9,
        out_specs=(any_spec,) * 4,
        scratch_shapes=[
            V((NT, D, T), bf), V((NT, D, T), bf), V((2, 3, FC, D), bf), V((4, D, 3 * FC), bf), V((3, D, FC), bf),
            V((3 * FC, D), bf), V((NT, D, T), f32), V((2, 3, D, FC), f32),
            V((2 * FC, T), bf), V((FC, T), bf), V((2 * FC, T), bf), V((FC, T), bf),
            V((4, RT, F), f32), V((6, 4, RT, FC), bf), V((6, 4, RT, FC), bf), V((6, 2, RT, FC), bf),
            V((6, 2, RT, FC), bf), V((6, RT, FC), bf), V((6, RT, FC), bf), V((6, RT, FC), bf),
            V((6, RT, FC), f32), V((6, RT, FC), f32), V((2, 6, RT, FC), f32), V((3, SH, D), f32),
            dma((2, NT)), dma((6,)), dma((4,)), dma((2,)), dma((NT,)), dma, dma((3,)), dma((93,)), dma((93,)),
        ],
        compiler_params=pltpu.CompilerParams(
            collective_id=0, has_side_effects=True, vmem_limit_bytes=67_000_000),
        cost_estimate=pl.CostEstimate(flops=43_500_000_000, bytes_accessed=60_000_000, transcendentals=4_718_592),
    )(xt, dyt, w1, w3, w2, v1, v3, v2, g)


def solution(mesh):
    def device_step(x_loc, dy_loc, w_gate, w_up, w_down, v_gate, v_up, v_down, g_next):
        dxt, dw, vo, gs = step_kernel(
            x_loc.T, dy_loc.T, w_gate.T, w_up.T, w_down, v_gate.T, v_up.T, v_down, g_next.reshape(3 * D, F))
        return dxt.T, gs.transpose(0, 2, 1), dw[None], vo[0], vo[1], vo[2].T

    row_spec = P(ALL_AXES, None)
    col_shard = P(None, FSDP_AXES)
    row_shard = P(FSDP_AXES, None)
    dev_spec = P(ALL_AXES, None, None, None)
    return jax.shard_map(
        device_step, mesh=mesh,
        in_specs=(row_spec, row_spec, col_shard, col_shard, row_shard, col_shard, col_shard, row_shard, dev_spec),
        out_specs=(row_spec, P(None, None, FSDP_AXES), dev_spec, P(), P(), P()),
        check_vma=False)
```

```python
import functools

import jax
import jax.numpy as jnp
from jax import lax
from jax.experimental import pallas as pl
from jax.experimental.pallas import tpu as pltpu
from jax.sharding import PartitionSpec as P

ALL_AXES = ('dp', 'col', 'fsdp')
FSDP_AXES = ('col', 'fsdp')
MESH = pl.DeviceIdType.MESH

D = 576
F = 1536
N = 3072
T = 512
NT = N // T
SH = 192
FC = 384
RT = 144
HR = D // 2
QR = HR // 2
NN = (((1,), (0,)), ((), ()))
NTD = (((1,), (1,)), ((), ()))

STEPS = {
    'AX': (0, 5, 7), 'AY': (0, 1, 2), 'BX': (7, 10, 13), 'BY': (5, 6, 8), 'CX': (9, 13, 15), 'CY': (8, 11, 14),
    'W1': (3,), 'WZ': (6,), 'WDA': (7,), 'WDB': (9,), 'W3': (16,), 'V': (13,), 'V1': (18, 20, 22),
    'D0': (11, 15, 17), 'D1': (10, 13, 16), 'E0': (15, 19, 22), 'E1': (13, 17, 20),
}


def dot(a, b, dn=NN):
    return lax.dot_general(a, b, dn, preferred_element_type=jnp.float32)


def kernel(xt, dyt, w1, w3, w2, v1, v3, v2, g, dxt, dw, vo, gs,
           ys, pair, blk, vblk, wt, dxa, dab0, hb0, dab1, hb1,
           gf, gb, gp, r1, r2, zb, z2, zs, tp,
           s_tok, s_loc, s_g, s_vo, ss, rs):
    xs = dxt
    z = lax.axis_index('dp')
    y = lax.axis_index('col')
    f = lax.axis_index('fsdp')
    x = f // 2
    k = f % 2
    own = 2 * y + x
    partner = (z, y, f + 1 - 2 * k)
    xn = (z, y, (f + 2) % 4)
    yn = (z, 1 - y, f)
    z_pair = z + 1 - 2 * (z % 2)
    zp = (z_pair, y, f)
    zm = (3 - z, y, f)
    at_end = (z == 0) | (z == 3)
    inner = (z == 1) | (z == 2)

    def rcopy(n, src, dst, dev):
        return pltpu.make_async_remote_copy(
            src_ref=src, dst_ref=dst, send_sem=ss.at[n], recv_sem=rs.at[n], device_id=dev, device_id_type=MESH)

    def tok(t):
        cols = pl.ds(pl.multiple_of(t * T, T), T)
        return (pltpu.make_async_copy(xt.at[:, cols], xs.at[:, cols], s_tok.at[0, t]),
                pltpu.make_async_copy(dyt.at[:, cols], ys.at[t], s_tok.at[1, t]))

    def g_tile(o):
        return jnp.where(o == 0, 0, jnp.where(o < 4, o + 2, o - 3))

    def gload(n):
        own_half = n >= 6
        o = jnp.where(own_half, n - 6, n)
        i = g_tile(o)
        h = jnp.where(own_half, k, 1 - k)
        r0 = pl.multiple_of(h * (6 * RT) + i * RT, RT)
        return pltpu.make_async_copy(g.at[pl.ds(r0, RT), :], gf.at[n % 4], s_g.at[n % 4])

    shards = ((w1, w3, w2), (v1, v3, v2))
    myrows = pl.ds(pl.multiple_of(k * SH, SH), SH)
    local_shards = [pltpu.make_async_copy(shards[u][m], pair.at[u, m, myrows, :], s_loc.at[3 * u + m])
                    for u in range(2) for m in range(3)]
    for n in range(4):
        gload(n).start()
    for c in local_shards:
        c.start()

    bar = pltpu.get_barrier_semaphore()
    for dev in (partner, xn, yn, zp, zm):
        pl.semaphore_signal(bar, inc=1, device_id=dev, device_id_type=MESH)
    pl.semaphore_wait(bar, 5)

    to_pair = [rcopy(3 * u + m, shards[u][m], pair.at[u, m, myrows, :], partner) for u in range(2) for m in range(3)]
    half = pl.ds(pl.multiple_of(k * HR, HR), HR)
    other = pl.ds(pl.multiple_of((1 - k) * HR, HR), HR)
    qa = pl.ds(pl.multiple_of(k * HR, QR), QR)
    qb = pl.ds(pl.multiple_of(k * HR + QR, QR), QR)

    def blkcols(cx, cy):
        xx = 1 - x if cx else x
        yy = 1 - y if cy else y
        return pl.ds(pl.multiple_of((2 * yy + xx) * FC, FC), FC)

    zo = z % 2
    qm = pl.ds(pl.multiple_of(k * HR + zo * QR, QR), QR)
    qo = pl.ds(pl.multiple_of(k * HR + (1 - zo) * QR, QR), QR)
    w_x = rcopy(6, blk.at[0, half, :], blk.at[1, half, :], xn)
    w_y = rcopy(7, blk.at[0, qm, :], blk.at[2, qm, :], yn)
    w_zy = rcopy(9, blk.at[2, qm, :], blk.at[2, qm, :], zp)
    w_f1 = rcopy(62, blk.at[1, half, :], blk.at[1, half, :], partner)
    w_f2a = rcopy(64, blk.at[2, qm, :], blk.at[2, qm, :], partner)
    w_f2b = rcopy(65, blk.at[2, qo, :], blk.at[2, qo, :], partner)
    w_da = rcopy(10, blk.at[1, qa, :], blk.at[3, qa, :], yn)
    w_db = rcopy(11, blk.at[2, qb, :], blk.at[3, qb, :], xn)
    w_f3 = rcopy(12, blk.at[3, half, :], blk.at[3, half, :], partner)

    v_own = pltpu.make_async_copy(vblk, vo.at[:, :, blkcols(0, 0)], s_vo)
    def v_copies(m):
        n = 66 + 7 * m
        q0, q1, q2, q3 = blkcols(0, 0), blkcols(1, 0), blkcols(0, 1), blkcols(1, 1)
        return (rcopy(n, vblk.at[m, half, :], vo.at[m, half, q0], xn),
                rcopy(n + 1, vblk.at[m, half, :], vo.at[m, half, q0], yn),
                rcopy(n + 2, vo.at[m, half, q1], vo.at[m, half, q1], partner),
                rcopy(n + 3, vo.at[m, half, q2], vo.at[m, half, q2], partner),
                rcopy(n + 4, vo.at[m, qa, q1], vo.at[m, qa, q1], yn),
                rcopy(n + 5, vo.at[m, qb, q2], vo.at[m, qb, q2], xn),
                rcopy(n + 6, vo.at[m, half, q3], vo.at[m, half, q3], partner))

    def to_partner(i):
        return rcopy(20 + i, gb.at[i], gp.at[i], partner)

    def first_x(j, yy):
        return rcopy(26 + 2 * j + yy, gp.at[j, 2 * yy + 1 - x], r1.at[j, yy], xn)

    def first_y(j, xx):
        return rcopy(32 + 2 * j + xx, gp.at[3 + j, 2 * (1 - y) + xx], r1.at[3 + j, xx], yn)

    def second_y(j):
        return rcopy(38 + j, r1.at[j, 1 - y], r2.at[j], yn)

    def second_x(j):
        return rcopy(41 + j, r1.at[3 + j, 1 - x], r2.at[3 + j], xn)

    def z_in(i):
        return rcopy(44 + i, zb.at[i], zb.at[i], zp)

    def z_mid(i):
        return rcopy(50 + i, zs.at[i], z2.at[i], zm)

    def z_out(i):
        return rcopy(56 + i, z2.at[i], z2.at[i], zp)

    def t_pair(i):
        return rcopy(87 + i, z2.at[i], tp.at[i], partner)

    for c in to_pair:
        c.start()
    for t in range(NT):
        for c in tok(t):
            c.start()

    def send_half(n, _):
        i = g_tile(n)
        gload(n).wait()
        for q in range(4):
            gb[i, q] = gf[n % 4, :, q * FC:(q + 1) * FC].astype(jnp.bfloat16)
        to_partner(i).start()
        gload(n + 4).start()
        return 0

    lax.fori_loop(0, 2, send_half, 0)

    for m in range(3):
        local_shards[m].wait()
        to_pair[m].wait_recv()
        blk[0, :, m * FC:(m + 1) * FC] = pair[0, m].T
    w_x.start()
    w_y.start()
    lax.fori_loop(2, 6, send_half, 0)

    def own_tile(i):
        n = 6 + (0, 4, 5, 1, 2, 3)[i]
        gload(n).wait()
        to_partner(i).wait_recv()
        for q in range(4):
            gp[i, q] = (gp[i, q].astype(jnp.float32)
                        + gf[n % 4, :, q * FC:(q + 1) * FC].astype(jnp.bfloat16).astype(jnp.float32)
                        ).astype(jnp.bfloat16)
        if n + 4 < 12:
            gload(n + 4).start()

    def stage_ax(j):
        own_tile(j)
        for b in range(2):
            first_x(j, b).start()

    def stage_ay(j):
        own_tile(3 + j)
        for b in range(2):
            first_y(j, b).start()

    def stage_bx(j):
        for b in range(2):
            first_x(j, b).wait_recv()
            r1[j, b] = (gp[j, 2 * b + x].astype(jnp.float32) + r1[j, b].astype(jnp.float32)).astype(jnp.bfloat16)
        second_y(j).start()

    def stage_by(j):
        for b in range(2):
            first_y(j, b).wait_recv()
            r1[3 + j, b] = (gp[3 + j, 2 * y + b].astype(jnp.float32)
                            + r1[3 + j, b].astype(jnp.float32)).astype(jnp.bfloat16)
        second_x(j).start()

    def second(i):
        return second_y(i) if i < 3 else second_x(i - 3)

    def mine(i):
        return y if i < 3 else x

    def stage_c(i):
        @pl.when(at_end)
        def _():
            second(i).wait_recv()
            zb[i] = (r1[i, mine(i)].astype(jnp.float32) + r2[i].astype(jnp.float32)).astype(jnp.bfloat16)
            z_in(i).start()

    def stage_d(i):
        @pl.when(inner)
        def _():
            second(i).wait_recv()
            z_in(i).wait_recv()
            zs[i] = (r1[i, mine(i)].astype(jnp.float32) + r2[i].astype(jnp.float32)) + zb[i].astype(jnp.float32)
            z_mid(i).start()

    def stage_e(i):
        @pl.when(inner)
        def _():
            z_mid(i).wait_recv()
            z2[i] = zs[i] + z2[i]
            z_out(i).start()
            t_pair(i).start()

    def v_start():
        for m in range(3):
            local_shards[3 + m].wait()
            to_pair[3 + m].wait_recv()
            vblk[m] = pair[1, m].T
            v_copies(m)[0].start()
            v_copies(m)[1].start()
        v_own.start()

    def w_1():
        w_y.wait_recv()
        w_zy.start()
        w_f2a.start()

    def w_z():
        w_zy.wait_recv()
        w_f2b.start()

    def w_3():
        w_da.wait_recv()
        w_db.wait_recv()
        w_f3.start()

    def v_1(m):
        v_x, v_y, v_f1, v_f2, v_da, v_db, _ = v_copies(m)
        v_x.wait_recv()
        v_da.start()
        v_f1.start()
        v_y.wait_recv()
        v_db.start()
        v_f2.start()

    def v_2(m):
        v_da, v_db, v_f3 = v_copies(m)[4:]
        v_da.wait_recv()
        v_db.wait_recv()
        v_f3.start()

    stages = {
        'AX': stage_ax, 'AY': stage_ay, 'BX': stage_bx, 'BY': stage_by,
        'CX': stage_c, 'CY': lambda j: stage_c(3 + j),
        'D0': stage_d, 'D1': lambda j: stage_d(3 + j), 'E0': stage_e, 'E1': lambda j: stage_e(3 + j),
        'V': lambda j: v_start(), 'V1': v_1,
        'W1': lambda j: w_1(), 'WZ': lambda j: w_z(), 'WDA': lambda j: w_da.start(), 'WDB': lambda j: w_db.start(),
        'W3': lambda j: w_3(),
    }
    order = ('W1', 'WZ', 'W3', 'BX', 'BY', 'AX', 'AY', 'CX', 'CY', 'D0', 'D1', 'E0', 'E1', 'WDA', 'WDB', 'V', 'V1')

    def tick(step, steps):
        for name in order:
            for j, n in enumerate(STEPS[name]):
                if n in steps:
                    if len(steps) == 1:
                        stages[name](j)
                    else:
                        pl.when(step == n)(functools.partial(stages[name], j))

    def dw_cols(c):
        cx, cy = c % 2, c // 2
        q = 2 * (y + cy - 2 * y * cy) + x + cx - 2 * x * cx
        return pl.ds(pl.multiple_of(q * FC, FC), FC)

    def head(c):
        @pl.when(c == 1)
        def _():
            w_x.wait_recv()
            w_f1.start()
            w_f1.wait_recv()

        @pl.when(c == 2)
        def _():
            w_f2a.wait_recv()
            w_f2b.wait_recv()

        @pl.when(c == 3)
        def _():
            w_f3.wait_recv()

        for m in range(3):
            wt[m * FC:(m + 1) * FC, :] = blk[c, :, m * FC:(m + 1) * FC].T

        dw[:, :, dw_cols(c)] = jnp.zeros((3, D, FC), jnp.float32)

    def first_touch(t):
        for cp in tok(t):
            cp.wait()
        dxa[t] = jnp.zeros((D, T), jnp.float32)

    def tcols(t):
        return pl.ds(pl.multiple_of(t * T, T), T)

    def forward(t, dab, hb):
        xv = xs[:, tcols(t)]
        a = dot(wt[0:FC, :], xv)
        b = dot(wt[FC:2 * FC, :], xv)
        dh = dot(wt[2 * FC:3 * FC, :], ys[t])
        sg = jnp.tanh(a * 0.5) * 0.5 + 0.5
        act = a * sg
        hb[...] = (act * b).astype(jnp.bfloat16)
        dab[FC:, :] = (dh * act).astype(jnp.bfloat16)
        dab[:FC, :] = (dh * b * (sg + act * (1.0 - sg))).astype(jnp.bfloat16)

    def backward(step, dab, hb):
        c, t = step // NT, step % NT
        dxa[t] += dot(blk[c, :, :2 * FC], dab[...])
        gw = dot(xs[:, tcols(t)], dab[...], NTD)
        cols = dw_cols(c)
        dw[0, :, cols] += gw[:, :FC]
        dw[1, :, cols] += gw[:, FC:]
        dw[2, :, cols] += dot(ys[t], hb[...], NTD)

    def half_step(step, steps, src, dst):
        c, t = step // NT, step % NT
        if any(n % NT == 0 for n in steps):
            @pl.when(t == 0)
            def _():
                head(c)

        if any(n < NT for n in steps):
            @pl.when(c == 0)
            def _():
                first_touch(t)

        tick(step, steps)
        forward(t, *dst)
        backward(step - 1, *src)

    b0, b1 = (dab0, hb0), (dab1, hb1)
    head(0)
    first_touch(0)
    tick(0, (0,))
    forward(0, *b0)

    def two_steps(p, _):
        half_step(2 * p + 1, tuple(range(1, 23, 2)), b0, b1)
        half_step(2 * p + 2, tuple(range(2, 23, 2)), b1, b0)
        return 0

    lax.fori_loop(0, 11, two_steps, 0)
    half_step(23, (23,), b0, b1)
    backward(23, *b1)

    def write_dx(t, _):
        xs[:, tcols(t)] = dxa[t].astype(jnp.bfloat16)
        return 0

    lax.fori_loop(0, NT, write_dx, 0)

    for name in order:
        for j, n in enumerate(STEPS[name]):
            if n >= 24:
                stages[name](j)

    for m in range(3):
        v_2(m)
    for i in (0, 3, 1, 4, 2, 5):
        @pl.when(at_end)
        def _():
            z_out(i).wait_recv()
            t_pair(i).start()
    for i in range(6):
        t_pair(i).wait_recv()

    for m in range(3):
        for kk in range(2):
            @pl.when(k == kk)
            def _():
                tiles = []
                for r in range(4 * m, 4 * m + 4):
                    src = z2 if r // 6 == kk else tp
                    tiles.append(src[r % 6])
                full = jnp.concatenate(tiles, axis=0).T
                gs[m] = full[kk * SH:(kk + 1) * SH]

    v_own.wait()
    for i in range(6):
        t_pair(i).wait_send()
        to_partner(i).wait_send()

        @pl.when(at_end)
        def _():
            z_in(i).wait_send()

        @pl.when(inner)
        def _():
            z_mid(i).wait_send()
            z_out(i).wait_send()
    for j in range(3):
        for b in range(2):
            first_x(j, b).wait_send()
            first_y(j, b).wait_send()
        second_x(j).wait_send()
        second_y(j).wait_send()
    for c in to_pair:
        c.wait_send()
    for c in (w_x, w_y, w_zy, w_f1, w_f2a, w_f2b, w_da, w_db, w_f3):
        c.wait_send()
    for m in range(3):
        for c in v_copies(m):
            c.wait_send()
        for c in (v_copies(m)[2], v_copies(m)[3], v_copies(m)[6]):
            c.wait_recv()


def step_kernel(xt, dyt, w1, w3, w2, v1, v3, v2, g):
    any_spec = pl.BlockSpec(memory_space=pl.ANY)
    vmem = pl.BlockSpec(memory_space=pltpu.VMEM)
    bf, f32 = jnp.bfloat16, jnp.float32
    V = pltpu.VMEM
    dma = pltpu.SemaphoreType.DMA
    return pl.pallas_call(
        kernel,
        name='mlp_step',
        out_shape=(V((D, N), bf), V((3, D, F), f32), jax.ShapeDtypeStruct((3, D, F), bf), V((3, SH, D), f32)),
        in_specs=[any_spec] * 9,
        out_specs=(vmem, vmem, any_spec, vmem),
        scratch_shapes=[
            V((NT, D, T), bf), V((2, 3, FC, D), bf), V((4, D, 3 * FC), bf), V((3, D, FC), bf),
            V((3 * FC, D), bf), V((NT, D, T), f32),
            V((2 * FC, T), bf), V((FC, T), bf), V((2 * FC, T), bf), V((FC, T), bf),
            V((4, RT, F), f32), V((6, 4, RT, FC), bf), V((6, 4, RT, FC), bf), V((6, 2, RT, FC), bf),
            V((6, RT, FC), bf), V((6, RT, FC), bf), V((6, RT, FC), f32), V((6, RT, FC), f32), V((6, RT, FC), f32),
            dma((2, NT)), dma((6,)), dma((4,)), dma, dma((93,)), dma((93,)),
        ],
        compiler_params=pltpu.CompilerParams(
            collective_id=0, has_side_effects=True, vmem_limit_bytes=50_800_000),
        cost_estimate=pl.CostEstimate(flops=43_500_000_000, bytes_accessed=60_000_000, transcendentals=4_718_592),
    )(xt, dyt, w1, w3, w2, v1, v3, v2, g)


def solution(mesh):
    def device_step(x_loc, dy_loc, w_gate, w_up, w_down, v_gate, v_up, v_down, g_next):
        dxt, dw, vo, gs = step_kernel(
            x_loc.T, dy_loc.T, w_gate.T, w_up.T, w_down, v_gate.T, v_up.T, v_down, g_next.reshape(3 * D, F))
        return dxt.T, gs.transpose(0, 2, 1), dw[None], vo[0], vo[1], vo[2].T

    row_spec = P(ALL_AXES, None)
    col_shard = P(None, FSDP_AXES)
    row_shard = P(FSDP_AXES, None)
    dev_spec = P(ALL_AXES, None, None, None)
    return jax.shard_map(
        device_step, mesh=mesh,
        in_specs=(row_spec, row_spec, col_shard, col_shard, row_shard, col_shard, col_shard, row_shard, dev_spec),
        out_specs=(row_spec, P(None, None, FSDP_AXES), dev_spec, P(), P(), P()),
        check_vma=False)
```

```python
import functools

import jax
import jax.numpy as jnp
from jax import lax
from jax.experimental import pallas as pl
from jax.experimental.pallas import tpu as pltpu
from jax.sharding import PartitionSpec as P

ALL_AXES = ('dp', 'col', 'fsdp')
FSDP_AXES = ('col', 'fsdp')
MESH = pl.DeviceIdType.MESH

D = 576
F = 1536
N = 3072
T = 512
NT = N // T
SH = 192
FC = 384
RT = 144
HR = D // 2
QR = HR // 2
NN = (((1,), (0,)), ((), ()))
NTD = (((1,), (1,)), ((), ()))

STEPS = {
    'AX': (4, 5, 7), 'AY': (0, 1, 2), 'BX': (7, 10, 12), 'BY': (5, 6, 8), 'CX': (9, 12, 14), 'CY': (8, 11, 13),
    'W1': (3,), 'WZ': (7,), 'WDA': (7,), 'WDB': (9,), 'W3': (16,), 'V': (13,), 'V1': (18, 19, 21), 'V2': (22, 23),
    'D0': (11, 14, 16), 'D1': (10, 13, 15), 'E0': (15, 18, 21), 'E1': (13, 16, 20),
    'F0': (18, 21, 24), 'F1': (16, 19, 23),
}


def dot(a, b, dn=NN):
    return lax.dot_general(a, b, dn, preferred_element_type=jnp.float32)


def kernel(xt, dyt, w1, w3, w2, v1, v3, v2, g, dxt, dw, vo, gs,
           ys, pair, blk, vblk, wt, dxa, dab0, hb0, dab1, hb1,
           gf, gb, gp, r1, r2, zb, z2, zs, tp,
           s_tok, s_loc, s_g, s_vo, ss, rs):
    xs = dxt
    z = lax.axis_index('dp')
    y = lax.axis_index('col')
    f = lax.axis_index('fsdp')
    x = f // 2
    k = f % 2
    own = 2 * y + x
    partner = (z, y, f + 1 - 2 * k)
    xn = (z, y, (f + 2) % 4)
    yn = (z, 1 - y, f)
    z_pair = z + 1 - 2 * (z % 2)
    zp = (z_pair, y, f)
    zm = (3 - z, y, f)
    at_end = (z == 0) | (z == 3)
    inner = (z == 1) | (z == 2)

    def rcopy(n, src, dst, dev):
        return pltpu.make_async_remote_copy(
            src_ref=src, dst_ref=dst, send_sem=ss.at[n], recv_sem=rs.at[n], device_id=dev, device_id_type=MESH)

    def tok(t):
        cols = pl.ds(pl.multiple_of(t * T, T), T)
        return (pltpu.make_async_copy(xt.at[:, cols], xs.at[:, cols], s_tok.at[0, t]),
                pltpu.make_async_copy(dyt.at[:, cols], ys.at[t], s_tok.at[1, t]))

    def g_tile(o):
        return jnp.where(o < 3, o + 3, o - 3)

    def gload(n):
        own_half = n >= 6
        o = jnp.where(own_half, n - 6, n)
        i = g_tile(o)
        h = jnp.where(own_half, k, 1 - k)
        r0 = pl.multiple_of(h * (6 * RT) + i * RT, RT)
        return pltpu.make_async_copy(g.at[pl.ds(r0, RT), :], gf.at[n % 4], s_g.at[n % 4])

    shards = ((w1, w3, w2), (v1, v3, v2))
    myrows = pl.ds(pl.multiple_of(k * SH, SH), SH)
    local_shards = [pltpu.make_async_copy(shards[u][m], pair.at[u, m, myrows, :], s_loc.at[3 * u + m])
                    for u in range(2) for m in range(3)]
    for n in range(4):
        gload(n).start()
    for c in local_shards:
        c.start()

    bar = pltpu.get_barrier_semaphore()
    for dev in (partner, xn, yn, zp, zm):
        pl.semaphore_signal(bar, inc=1, device_id=dev, device_id_type=MESH)
    pl.semaphore_wait(bar, 5)

    to_pair = [rcopy(3 * u + m, shards[u][m], pair.at[u, m, myrows, :], partner) for u in range(2) for m in range(3)]
    half = pl.ds(pl.multiple_of(k * HR, HR), HR)
    other = pl.ds(pl.multiple_of((1 - k) * HR, HR), HR)
    qa = pl.ds(pl.multiple_of(k * HR, QR), QR)
    qb = pl.ds(pl.multiple_of(k * HR + QR, QR), QR)

    def blkcols(cx, cy):
        xx = 1 - x if cx else x
        yy = 1 - y if cy else y
        return pl.ds(pl.multiple_of((2 * yy + xx) * FC, FC), FC)

    zo = z % 2
    qm = pl.ds(pl.multiple_of(k * HR + zo * QR, QR), QR)
    qo = pl.ds(pl.multiple_of(k * HR + (1 - zo) * QR, QR), QR)
    w_x = rcopy(6, blk.at[0, half, :], blk.at[1, half, :], xn)
    w_y = rcopy(7, blk.at[0, qm, :], blk.at[2, qm, :], yn)
    w_zy = rcopy(9, blk.at[2, qm, :], blk.at[2, qm, :], zp)
    w_f1 = rcopy(62, blk.at[1, half, :], blk.at[1, half, :], partner)
    w_f2a = rcopy(64, blk.at[2, qm, :], blk.at[2, qm, :], partner)
    w_f2b = rcopy(65, blk.at[2, qo, :], blk.at[2, qo, :], partner)
    w_da = rcopy(10, blk.at[1, qa, :], blk.at[3, qa, :], yn)
    w_db = rcopy(11, blk.at[2, qb, :], blk.at[3, qb, :], xn)
    w_f3 = rcopy(12, blk.at[3, half, :], blk.at[3, half, :], partner)

    v_own = pltpu.make_async_copy(vblk, vo.at[:, :, blkcols(0, 0)], s_vo)
    def v_copies(m):
        n = 66 + 7 * m
        q0, q1, q2, q3 = blkcols(0, 0), blkcols(1, 0), blkcols(0, 1), blkcols(1, 1)
        return (rcopy(n, vblk.at[m, half, :], vo.at[m, half, q0], xn),
                rcopy(n + 1, vblk.at[m, half, :], vo.at[m, half, q0], yn),
                rcopy(n + 2, vo.at[m, half, q1], vo.at[m, half, q1], partner),
                rcopy(n + 3, vo.at[m, half, q2], vo.at[m, half, q2], partner),
                rcopy(n + 4, vo.at[m, qa, q1], vo.at[m, qa, q1], yn),
                rcopy(n + 5, vo.at[m, qb, q2], vo.at[m, qb, q2], xn),
                rcopy(n + 6, vo.at[m, half, q3], vo.at[m, half, q3], partner))

    def to_partner(i):
        return rcopy(20 + i, gb.at[i], gp.at[i], partner)

    def first_x(j, yy):
        return rcopy(26 + 2 * j + yy, gp.at[j, 2 * yy + 1 - x], r1.at[j, yy], xn)

    def first_y(j, xx):
        return rcopy(32 + 2 * j + xx, gp.at[3 + j, 2 * (1 - y) + xx], r1.at[3 + j, xx], yn)

    def second_y(j):
        return rcopy(38 + j, r1.at[j, 1 - y], r2.at[j], yn)

    def second_x(j):
        return rcopy(41 + j, r1.at[3 + j, 1 - x], r2.at[3 + j], xn)

    def z_in(i):
        return rcopy(44 + i, zb.at[i], zb.at[i], zp)

    def z_mid(i):
        return rcopy(50 + i, zs.at[i], z2.at[i], zm)

    def z_out(i):
        return rcopy(56 + i, z2.at[i], z2.at[i], zp)

    def t_pair(i):
        return rcopy(87 + i, z2.at[i], tp.at[i], partner)

    for c in to_pair:
        c.start()
    for c in tok(0):
        c.start()

    def send_half(n, _):
        i = g_tile(n)
        gload(n).wait()
        for q in range(4):
            gb[i, q] = gf[n % 4, :, q * FC:(q + 1) * FC].astype(jnp.bfloat16)
        to_partner(i).start()
        gload(n + 4).start()
        return 0

    lax.fori_loop(0, 2, send_half, 0)

    for m in range(3):
        local_shards[m].wait()
        to_pair[m].wait_recv()
        blk[0, :, m * FC:(m + 1) * FC] = pair[0, m].T
    w_x.start()
    w_y.start()
    lax.fori_loop(2, 6, send_half, 0)
    for t in range(1, NT):
        for c in tok(t):
            c.start()

    def own_tile(i):
        n = 6 + (3, 4, 5, 0, 1, 2)[i]
        gload(n).wait()
        to_partner(i).wait_recv()
        for q in range(4):
            gp[i, q] = (gp[i, q].astype(jnp.float32)
                        + gf[n % 4, :, q * FC:(q + 1) * FC].astype(jnp.bfloat16).astype(jnp.float32)
                        ).astype(jnp.bfloat16)
        if n + 4 < 12:
            gload(n + 4).start()

    def stage_ax(j):
        own_tile(j)
        for b in range(2):
            first_x(j, b).start()

    def stage_ay(j):
        own_tile(3 + j)
        for b in range(2):
            first_y(j, b).start()

    def stage_bx(j):
        for b in range(2):
            first_x(j, b).wait_recv()
            r1[j, b] = (gp[j, 2 * b + x].astype(jnp.float32) + r1[j, b].astype(jnp.float32)).astype(jnp.bfloat16)
        second_y(j).start()

    def stage_by(j):
        for b in range(2):
            first_y(j, b).wait_recv()
            r1[3 + j, b] = (gp[3 + j, 2 * y + b].astype(jnp.float32)
                            + r1[3 + j, b].astype(jnp.float32)).astype(jnp.bfloat16)
        second_x(j).start()

    def second(i):
        return second_y(i) if i < 3 else second_x(i - 3)

    def mine(i):
        return y if i < 3 else x

    def stage_c(i):
        @pl.when(at_end)
        def _():
            second(i).wait_recv()
            zb[i] = (r1[i, mine(i)].astype(jnp.float32) + r2[i].astype(jnp.float32)).astype(jnp.bfloat16)
            z_in(i).start()

    def stage_d(i):
        @pl.when(inner)
        def _():
            second(i).wait_recv()
            z_in(i).wait_recv()
            zs[i] = (r1[i, mine(i)].astype(jnp.float32) + r2[i].astype(jnp.float32)) + zb[i].astype(jnp.float32)
            z_mid(i).start()

    def stage_e(i):
        @pl.when(inner)
        def _():
            z_mid(i).wait_recv()
            z2[i] = zs[i] + z2[i]
            z_out(i).start()
            t_pair(i).start()

    def stage_f(i):
        @pl.when(at_end)
        def _():
            z_out(i).wait_recv()
            t_pair(i).start()

    def v_start():
        for m in range(3):
            local_shards[3 + m].wait()
            to_pair[3 + m].wait_recv()
            vblk[m] = pair[1, m].T
            v_copies(m)[0].start()
            v_copies(m)[1].start()
        v_own.start()

    def w_1():
        w_y.wait_recv()
        w_zy.start()
        w_f2a.start()

    def w_z():
        w_zy.wait_recv()
        w_f2b.start()

    def w_3():
        w_da.wait_recv()
        w_db.wait_recv()
        w_f3.start()

    def v_1(m):
        v_x, v_y, v_f1, v_f2, v_da, v_db, _ = v_copies(m)
        v_x.wait_recv()
        v_da.start()
        v_f1.start()
        v_y.wait_recv()
        v_db.start()
        v_f2.start()

    def v_2(m):
        v_da, v_db, v_f3 = v_copies(m)[4:]
        v_da.wait_recv()
        v_db.wait_recv()
        v_f3.start()

    stages = {
        'AX': stage_ax, 'AY': stage_ay, 'BX': stage_bx, 'BY': stage_by,
        'CX': stage_c, 'CY': lambda j: stage_c(3 + j),
        'D0': stage_d, 'D1': lambda j: stage_d(3 + j), 'E0': stage_e, 'E1': lambda j: stage_e(3 + j),
        'F0': stage_f, 'F1': lambda j: stage_f(3 + j), 'V': lambda j: v_start(), 'V1': v_1, 'V2': v_2,
        'W1': lambda j: w_1(), 'WZ': lambda j: w_z(), 'WDA': lambda j: w_da.start(), 'WDB': lambda j: w_db.start(),
        'W3': lambda j: w_3(),
    }
    order = ('W1', 'WZ', 'W3', 'BX', 'BY', 'AX', 'AY', 'CX', 'CY', 'D0', 'D1', 'E0', 'E1', 'F0', 'F1', 'WDA', 'WDB', 'V', 'V1', 'V2')

    def tick(step, steps):
        for name in order:
            for j, n in enumerate(STEPS[name]):
                if n in steps:
                    if len(steps) == 1:
                        stages[name](j)
                    else:
                        pl.when(step == n)(functools.partial(stages[name], j))

    def dw_cols(c):
        cx, cy = c % 2, c // 2
        q = 2 * (y + cy - 2 * y * cy) + x + cx - 2 * x * cx
        return pl.ds(pl.multiple_of(q * FC, FC), FC)

    def head(c):
        @pl.when(c == 1)
        def _():
            w_x.wait_recv()
            w_f1.start()
            w_f1.wait_recv()

        @pl.when(c == 2)
        def _():
            w_f2a.wait_recv()
            w_f2b.wait_recv()

        @pl.when(c == 3)
        def _():
            w_f3.wait_recv()

        for m in range(3):
            wt[m * FC:(m + 1) * FC, :] = blk[c, :, m * FC:(m + 1) * FC].T

        dw[:, :, dw_cols(c)] = jnp.zeros((3, D, FC), jnp.float32)

    def first_touch(t):
        for cp in tok(t):
            cp.wait()
        dxa[t] = jnp.zeros((D, T), jnp.float32)

    def tcols(t):
        return pl.ds(pl.multiple_of(t * T, T), T)

    def forward(t, dab, hb):
        xv = xs[:, tcols(t)]
        a = dot(wt[0:FC, :], xv)
        b = dot(wt[FC:2 * FC, :], xv)
        dh = dot(wt[2 * FC:3 * FC, :], ys[t])
        sg = jnp.tanh(a * 0.5) * 0.5 + 0.5
        act = a * sg
        hb[...] = (act * b).astype(jnp.bfloat16)
        dab[FC:, :] = (dh * act).astype(jnp.bfloat16)
        dab[:FC, :] = (dh * b * (sg + act * (1.0 - sg))).astype(jnp.bfloat16)

    def backward(step, dab, hb):
        c, t = step // NT, step % NT
        dxa[t] += dot(blk[c, :, :2 * FC], dab[...])
        gw = dot(xs[:, tcols(t)], dab[...], NTD)
        cols = dw_cols(c)
        dw[0, :, cols] += gw[:, :FC]
        dw[1, :, cols] += gw[:, FC:]
        dw[2, :, cols] += dot(ys[t], hb[...], NTD)

    def half_step(step, steps, src, dst):
        c, t = step // NT, step % NT
        if any(n % NT == 0 for n in steps):
            @pl.when(t == 0)
            def _():
                head(c)

        if any(n < NT for n in steps):
            @pl.when(c == 0)
            def _():
                first_touch(t)

        tick(step, steps)
        forward(t, *dst)
        backward(step - 1, *src)

    b0, b1 = (dab0, hb0), (dab1, hb1)
    head(0)
    first_touch(0)
    tick(0, (0,))
    forward(0, *b0)

    def two_steps(p, _):
        half_step(2 * p + 1, tuple(range(1, 23, 2)), b0, b1)
        half_step(2 * p + 2, tuple(range(2, 23, 2)), b1, b0)
        return 0

    lax.fori_loop(0, 11, two_steps, 0)
    half_step(23, (23,), b0, b1)
    v_2(2)
    backward(23, *b1)

    def write_dx(t, _):
        xs[:, tcols(t)] = dxa[t].astype(jnp.bfloat16)
        return 0

    lax.fori_loop(0, NT, write_dx, 0)

    for name in order:
        for j, n in enumerate(STEPS[name]):
            if n >= 24:
                stages[name](j)

    for i in range(6):
        t_pair(i).wait_recv()

    for m in range(3):
        for kk in range(2):
            @pl.when(k == kk)
            def _():
                tiles = []
                for r in range(4 * m, 4 * m + 4):
                    src = z2 if r // 6 == kk else tp
                    tiles.append(src[r % 6])
                full = jnp.concatenate(tiles, axis=0).T
                gs[m] = full[kk * SH:(kk + 1) * SH]

    v_own.wait()
    for i in range(6):
        t_pair(i).wait_send()
        to_partner(i).wait_send()

        @pl.when(at_end)
        def _():
            z_in(i).wait_send()

        @pl.when(inner)
        def _():
            z_mid(i).wait_send()
            z_out(i).wait_send()
    for j in range(3):
        for b in range(2):
            first_x(j, b).wait_send()
            first_y(j, b).wait_send()
        second_x(j).wait_send()
        second_y(j).wait_send()
    for c in to_pair:
        c.wait_send()
    for c in (w_x, w_y, w_zy, w_f1, w_f2a, w_f2b, w_da, w_db, w_f3):
        c.wait_send()
    for m in range(3):
        for c in v_copies(m):
            c.wait_send()
        for c in (v_copies(m)[2], v_copies(m)[3], v_copies(m)[6]):
            c.wait_recv()


def step_kernel(xt, dyt, w1, w3, w2, v1, v3, v2, g):
    any_spec = pl.BlockSpec(memory_space=pl.ANY)
    vmem = pl.BlockSpec(memory_space=pltpu.VMEM)
    bf, f32 = jnp.bfloat16, jnp.float32
    V = pltpu.VMEM
    dma = pltpu.SemaphoreType.DMA
    return pl.pallas_call(
        kernel,
        name='mlp_step',
        out_shape=(V((D, N), bf), V((3, D, F), f32), jax.ShapeDtypeStruct((3, D, F), bf), V((3, SH, D), f32)),
        in_specs=[any_spec] * 9,
        out_specs=(vmem, vmem, any_spec, vmem),
        scratch_shapes=[
            V((NT, D, T), bf), V((2, 3, FC, D), bf), V((4, D, 3 * FC), bf), V((3, D, FC), bf),
            V((3 * FC, D), bf), V((NT, D, T), f32),
            V((2 * FC, T), bf), V((FC, T), bf), V((2 * FC, T), bf), V((FC, T), bf),
            V((4, RT, F), f32), V((6, 4, RT, FC), bf), V((6, 4, RT, FC), bf), V((6, 2, RT, FC), bf),
            V((6, RT, FC), bf), V((6, RT, FC), bf), V((6, RT, FC), f32), V((6, RT, FC), f32), V((6, RT, FC), f32),
            dma((2, NT)), dma((6,)), dma((4,)), dma, dma((93,)), dma((93,)),
        ],
        compiler_params=pltpu.CompilerParams(
            collective_id=0, has_side_effects=True, vmem_limit_bytes=50_800_000),
        cost_estimate=pl.CostEstimate(flops=43_500_000_000, bytes_accessed=60_000_000, transcendentals=4_718_592),
    )(xt, dyt, w1, w3, w2, v1, v3, v2, g)


def solution(mesh):
    def device_step(x_loc, dy_loc, w_gate, w_up, w_down, v_gate, v_up, v_down, g_next):
        dxt, dw, vo, gs = step_kernel(
            x_loc.T, dy_loc.T, w_gate.T, w_up.T, w_down, v_gate.T, v_up.T, v_down, g_next.reshape(3 * D, F))
        return dxt.T, gs.transpose(0, 2, 1), dw[None], vo[0], vo[1], vo[2].T

    row_spec = P(ALL_AXES, None)
    col_shard = P(None, FSDP_AXES)
    row_shard = P(FSDP_AXES, None)
    dev_spec = P(ALL_AXES, None, None, None)
    return jax.shard_map(
        device_step, mesh=mesh,
        in_specs=(row_spec, row_spec, col_shard, col_shard, row_shard, col_shard, col_shard, row_shard, dev_spec),
        out_specs=(row_spec, P(None, None, FSDP_AXES), dev_spec, P(), P(), P()),
        check_vma=False)
```

```python
import functools

import jax
import jax.numpy as jnp
from jax import lax
from jax.experimental import pallas as pl
from jax.experimental.pallas import tpu as pltpu
from jax.sharding import PartitionSpec as P

ALL_AXES = ('dp', 'col', 'fsdp')
FSDP_AXES = ('col', 'fsdp')
MESH = pl.DeviceIdType.MESH

D = 576
F = 1536
N = 3072
T = 512
NT = N // T
SH = 192
FC = 384
RT = 144
HR = D // 2
QR = HR // 2
NN = (((1,), (0,)), ((), ()))
NTD = (((1,), (1,)), ((), ()))

STEPS = {
    'AX': (4, 5, 7), 'AY': (0, 1, 2), 'BX': (7, 10, 12), 'BY': (5, 6, 8), 'CX': (9, 12, 14), 'CY': (8, 11, 13),
    'W1': (4,), 'WZ': (7,), 'WDA': (7,), 'WDB': (9,), 'W3': (16,), 'V': (13,), 'V1': (18, 19, 21), 'V2': (22, 23),
    'D0': (11, 14, 16), 'D1': (10, 13, 15), 'E0': (15, 18, 21), 'E1': (13, 16, 20),
    'F0': (18, 21, 24), 'F1': (16, 19, 23),
}


def dot(a, b, dn=NN):
    return lax.dot_general(a, b, dn, preferred_element_type=jnp.float32)


def kernel(xt, dyt, w1, w3, w2, v1, v3, v2, g, dxt, dw, vo, gs,
           ys, pair, blk, wt, dxa, dab0, hb0, dab1, hb1,
           gf, gb, gp, r1, r2, zb, z2, zs, tp,
           s_tok, s_loc, s_g, ss, rs):
    xs = dxt
    z = lax.axis_index('dp')
    y = lax.axis_index('col')
    f = lax.axis_index('fsdp')
    x = f // 2
    k = f % 2
    own = 2 * y + x
    partner = (z, y, f + 1 - 2 * k)
    xn = (z, y, (f + 2) % 4)
    yn = (z, 1 - y, f)
    z_pair = z + 1 - 2 * (z % 2)
    zp = (z_pair, y, f)
    zm = (3 - z, y, f)
    at_end = (z == 0) | (z == 3)
    inner = (z == 1) | (z == 2)

    def rcopy(n, src, dst, dev):
        return pltpu.make_async_remote_copy(
            src_ref=src, dst_ref=dst, send_sem=ss.at[n], recv_sem=rs.at[n], device_id=dev, device_id_type=MESH)

    def tok(t):
        cols = pl.ds(pl.multiple_of(t * T, T), T)
        return (pltpu.make_async_copy(xt.at[:, cols], xs.at[:, cols], s_tok.at[0, t]),
                pltpu.make_async_copy(dyt.at[:, cols], ys.at[t], s_tok.at[1, t]))

    def g_tile(o):
        return jnp.where(o < 3, o + 3, o - 3)

    def gload(n):
        own_half = n >= 6
        o = jnp.where(own_half, n - 6, n)
        i = g_tile(o)
        h = jnp.where(own_half, k, 1 - k)
        r0 = pl.multiple_of(h * (6 * RT) + i * RT, RT)
        return pltpu.make_async_copy(g.at[pl.ds(r0, RT), :], gf.at[n % 4], s_g.at[n % 4])

    shards = ((w1, w3, w2), (v1, v3, v2))
    myrows = pl.ds(pl.multiple_of(k * SH, SH), SH)
    local_shards = [pltpu.make_async_copy(shards[u][m], pair.at[u, m, myrows, :], s_loc.at[3 * u + m])
                    for u in range(2) for m in range(3)]
    for n in range(4):
        gload(n).start()
    for c in local_shards:
        c.start()

    bar = pltpu.get_barrier_semaphore()
    for dev in (partner, xn, yn, zp, zm):
        pl.semaphore_signal(bar, inc=1, device_id=dev, device_id_type=MESH)
    pl.semaphore_wait(bar, 5)

    to_pair = [rcopy(3 * u + m, shards[u][m], pair.at[u, m, myrows, :], partner) for u in range(2) for m in range(3)]
    half = pl.ds(pl.multiple_of(k * HR, HR), HR)
    other = pl.ds(pl.multiple_of((1 - k) * HR, HR), HR)
    qa = pl.ds(pl.multiple_of(k * HR, QR), QR)
    qb = pl.ds(pl.multiple_of(k * HR + QR, QR), QR)

    def blkcols(cx, cy):
        xx = 1 - x if cx else x
        yy = 1 - y if cy else y
        return pl.ds(pl.multiple_of((2 * yy + xx) * FC, FC), FC)

    zo = z % 2
    qm = pl.ds(pl.multiple_of(k * HR + zo * QR, QR), QR)
    qo = pl.ds(pl.multiple_of(k * HR + (1 - zo) * QR, QR), QR)
    w_x = rcopy(6, blk.at[0, half, :], blk.at[1, half, :], xn)
    w_y = rcopy(7, blk.at[0, qm, :], blk.at[2, qm, :], yn)
    w_zy = rcopy(9, blk.at[2, qm, :], blk.at[2, qm, :], zp)
    w_f1 = rcopy(62, blk.at[1, half, :], blk.at[1, half, :], partner)
    w_f2a = rcopy(64, blk.at[2, qm, :], blk.at[2, qm, :], partner)
    w_f2b = rcopy(65, blk.at[2, qo, :], blk.at[2, qo, :], partner)
    w_da = rcopy(10, blk.at[1, qa, :], blk.at[3, qa, :], yn)
    w_db = rcopy(11, blk.at[2, qb, :], blk.at[3, qb, :], xn)
    w_f3 = rcopy(12, blk.at[3, half, :], blk.at[3, half, :], partner)

    def v_copies(m):
        n = 66 + 7 * m
        q0, q1, q2, q3 = blkcols(0, 0), blkcols(1, 0), blkcols(0, 1), blkcols(1, 1)
        return (rcopy(n, vo.at[m, half, q0], vo.at[m, half, q0], xn),
                rcopy(n + 1, vo.at[m, half, q0], vo.at[m, half, q0], yn),
                rcopy(n + 2, vo.at[m, half, q1], vo.at[m, half, q1], partner),
                rcopy(n + 3, vo.at[m, half, q2], vo.at[m, half, q2], partner),
                rcopy(n + 4, vo.at[m, qa, q1], vo.at[m, qa, q1], yn),
                rcopy(n + 5, vo.at[m, qb, q2], vo.at[m, qb, q2], xn),
                rcopy(n + 6, vo.at[m, half, q3], vo.at[m, half, q3], partner))

    def to_partner(i):
        return rcopy(20 + i, gb.at[i], gp.at[i], partner)

    def first_x(j, yy):
        return rcopy(26 + 2 * j + yy, gp.at[j, 2 * yy + 1 - x], r1.at[j, yy], xn)

    def first_y(j, xx):
        return rcopy(32 + 2 * j + xx, gp.at[3 + j, 2 * (1 - y) + xx], r1.at[3 + j, xx], yn)

    def second_y(j):
        return rcopy(38 + j, r1.at[j, 1 - y], r2.at[j], yn)

    def second_x(j):
        return rcopy(41 + j, r1.at[3 + j, 1 - x], r2.at[3 + j], xn)

    def z_in(i):
        return rcopy(44 + i, zb.at[i], zb.at[i], zp)

    def z_mid(i):
        return rcopy(50 + i, zs.at[i], z2.at[i], zm)

    def z_out(i):
        return rcopy(56 + i, z2.at[i], z2.at[i], zp)

    def t_pair(i):
        return rcopy(87 + i, z2.at[i], tp.at[i], partner)

    for c in to_pair:
        c.start()
    for c in tok(0):
        c.start()

    def send_half(n, _):
        i = g_tile(n)
        gload(n).wait()
        for q in range(4):
            gb[i, q] = gf[n % 4, :, q * FC:(q + 1) * FC].astype(jnp.bfloat16)
        to_partner(i).start()
        gload(n + 4).start()
        return 0

    lax.fori_loop(0, 2, send_half, 0)

    for m in range(3):
        local_shards[m].wait()
        to_pair[m].wait_recv()
        blk[0, :, m * FC:(m + 1) * FC] = pair[0, m].T
    w_x.start()
    w_y.start()
    lax.fori_loop(2, 6, send_half, 0)
    for t in range(1, NT):
        for c in tok(t):
            c.start()

    def own_tile(i):
        n = 6 + (3, 4, 5, 0, 1, 2)[i]
        gload(n).wait()
        to_partner(i).wait_recv()
        for q in range(4):
            gp[i, q] = (gp[i, q].astype(jnp.float32)
                        + gf[n % 4, :, q * FC:(q + 1) * FC].astype(jnp.bfloat16).astype(jnp.float32)
                        ).astype(jnp.bfloat16)
        if n + 4 < 12:
            gload(n + 4).start()

    def stage_ax(j):
        own_tile(j)
        for b in range(2):
            first_x(j, b).start()

    def stage_ay(j):
        own_tile(3 + j)
        for b in range(2):
            first_y(j, b).start()

    def stage_bx(j):
        for b in range(2):
            first_x(j, b).wait_recv()
            r1[j, b] = (gp[j, 2 * b + x].astype(jnp.float32) + r1[j, b].astype(jnp.float32)).astype(jnp.bfloat16)
        second_y(j).start()

    def stage_by(j):
        for b in range(2):
            first_y(j, b).wait_recv()
            r1[3 + j, b] = (gp[3 + j, 2 * y + b].astype(jnp.float32)
                            + r1[3 + j, b].astype(jnp.float32)).astype(jnp.bfloat16)
        second_x(j).start()

    def second(i):
        return second_y(i) if i < 3 else second_x(i - 3)

    def mine(i):
        return y if i < 3 else x

    def stage_c(i):
        @pl.when(at_end)
        def _():
            second(i).wait_recv()
            zb[i] = (r1[i, mine(i)].astype(jnp.float32) + r2[i].astype(jnp.float32)).astype(jnp.bfloat16)
            z_in(i).start()

    def stage_d(i):
        @pl.when(inner)
        def _():
            second(i).wait_recv()
            z_in(i).wait_recv()
            zs[i] = (r1[i, mine(i)].astype(jnp.float32) + r2[i].astype(jnp.float32)) + zb[i].astype(jnp.float32)
            z_mid(i).start()

    def stage_e(i):
        @pl.when(inner)
        def _():
            z_mid(i).wait_recv()
            z2[i] = zs[i] + z2[i]
            z_out(i).start()
            t_pair(i).start()

    def stage_f(i):
        @pl.when(at_end)
        def _():
            z_out(i).wait_recv()
            t_pair(i).start()

    def v_turn():
        for m in range(3):
            local_shards[3 + m].wait()
            to_pair[3 + m].wait_recv()
            vo[m, :, blkcols(0, 0)] = pair[1, m].T

    def v_start():
        for m in range(3):
            v_copies(m)[0].start()
            v_copies(m)[1].start()

    def w_1():
        w_y.wait_recv()
        w_zy.start()
        w_f2a.start()

    def w_z():
        w_zy.wait_recv()
        w_f2b.start()

    def w_3():
        w_da.wait_recv()
        w_db.wait_recv()
        w_f3.start()

    def v_1(m):
        v_x, v_y, v_f1, v_f2, v_da, v_db, _ = v_copies(m)
        v_x.wait_recv()
        v_da.start()
        v_f1.start()
        v_y.wait_recv()
        v_db.start()
        v_f2.start()

    def v_2(m):
        v_da, v_db, v_f3 = v_copies(m)[4:]
        v_da.wait_recv()
        v_db.wait_recv()
        v_f3.start()

    stages = {
        'AX': stage_ax, 'AY': stage_ay, 'BX': stage_bx, 'BY': stage_by,
        'CX': stage_c, 'CY': lambda j: stage_c(3 + j),
        'D0': stage_d, 'D1': lambda j: stage_d(3 + j), 'E0': stage_e, 'E1': lambda j: stage_e(3 + j),
        'F0': stage_f, 'F1': lambda j: stage_f(3 + j), 'V': lambda j: v_start(), 'V1': v_1, 'V2': v_2,
        'W1': lambda j: w_1(), 'WZ': lambda j: w_z(), 'WDA': lambda j: w_da.start(), 'WDB': lambda j: w_db.start(),
        'W3': lambda j: w_3(),
    }
    order = ('W1', 'WZ', 'W3', 'BX', 'BY', 'AX', 'AY', 'CX', 'CY', 'D0', 'D1', 'E0', 'E1', 'F0', 'F1', 'WDA', 'WDB', 'V', 'V1', 'V2')

    def tick(step, steps):
        for name in order:
            for j, n in enumerate(STEPS[name]):
                if n in steps:
                    if len(steps) == 1:
                        stages[name](j)
                    else:
                        pl.when(step == n)(functools.partial(stages[name], j))

    def dw_cols(c):
        cx, cy = c % 2, c // 2
        q = 2 * (y + cy - 2 * y * cy) + x + cx - 2 * x * cx
        return pl.ds(pl.multiple_of(q * FC, FC), FC)

    def head(c):
        dw[:, :, dw_cols(c)] = jnp.zeros((3, D, FC), jnp.float32)

        @pl.when(c == 1)
        def _():
            w_x.wait_recv()
            w_f1.start()
            v_turn()
            w_f1.wait_recv()

        @pl.when(c == 2)
        def _():
            w_f2a.wait_recv()
            w_f2b.wait_recv()

        @pl.when(c == 3)
        def _():
            w_f3.wait_recv()

        for m in range(3):
            rows = slice(m * FC, (m + 1) * FC)
            wt[rows, :] = pair[0, m] if isinstance(c, int) else blk[c, :, rows].T

    def first_touch(t):
        for cp in tok(t):
            cp.wait()
        dxa[t] = jnp.zeros((D, T), jnp.float32)

    def tcols(t):
        return pl.ds(pl.multiple_of(t * T, T), T)

    def forward(t, dab, hb):
        xv = xs[:, tcols(t)]
        a = dot(wt[0:FC, :], xv)
        b = dot(wt[FC:2 * FC, :], xv)
        dh = dot(wt[2 * FC:3 * FC, :], ys[t])
        sg = jnp.tanh(a * 0.5) * 0.5 + 0.5
        act = a * sg
        hb[...] = (act * b).astype(jnp.bfloat16)
        dab[FC:, :] = (dh * act).astype(jnp.bfloat16)
        dab[:FC, :] = (dh * b * (sg + act * (1.0 - sg))).astype(jnp.bfloat16)

    def backward(step, dab, hb):
        c, t = step // NT, step % NT
        dxa[t] += dot(blk[c, :, :2 * FC], dab[...])
        gw = dot(xs[:, tcols(t)], dab[...], NTD)
        cols = dw_cols(c)
        dw[0, :, cols] += gw[:, :FC]
        dw[1, :, cols] += gw[:, FC:]
        dw[2, :, cols] += dot(ys[t], hb[...], NTD)

    def half_step(step, steps, src, dst):
        c, t = step // NT, step % NT
        if any(n % NT == 0 for n in steps):
            @pl.when(t == 0)
            def _():
                head(c)

        if any(n < NT for n in steps):
            @pl.when(c == 0)
            def _():
                first_touch(t)

        tick(step, steps)
        forward(t, *dst)
        backward(step - 1, *src)

    b0, b1 = (dab0, hb0), (dab1, hb1)
    head(0)
    first_touch(0)
    tick(0, (0,))
    forward(0, *b0)

    def two_steps(p, _):
        half_step(2 * p + 1, tuple(range(1, 23, 2)), b0, b1)
        half_step(2 * p + 2, tuple(range(2, 23, 2)), b1, b0)
        return 0

    lax.fori_loop(0, 11, two_steps, 0)
    half_step(23, (23,), b0, b1)
    v_2(2)
    backward(23, *b1)

    def write_dx(t, _):
        xs[:, tcols(t)] = dxa[t].astype(jnp.bfloat16)
        return 0

    lax.fori_loop(0, NT, write_dx, 0)

    for name in order:
        for j, n in enumerate(STEPS[name]):
            if n >= 24:
                stages[name](j)

    for i in range(6):
        t_pair(i).wait_recv()

    for m in range(3):
        for kk in range(2):
            @pl.when(k == kk)
            def _():
                tiles = []
                for r in range(4 * m, 4 * m + 4):
                    src = z2 if r // 6 == kk else tp
                    tiles.append(src[r % 6])
                full = jnp.concatenate(tiles, axis=0).T
                gs[m] = full[kk * SH:(kk + 1) * SH]

    for i in range(6):
        t_pair(i).wait_send()
        to_partner(i).wait_send()

        @pl.when(at_end)
        def _():
            z_in(i).wait_send()

        @pl.when(inner)
        def _():
            z_mid(i).wait_send()
            z_out(i).wait_send()
    for j in range(3):
        for b in range(2):
            first_x(j, b).wait_send()
            first_y(j, b).wait_send()
        second_x(j).wait_send()
        second_y(j).wait_send()
    for c in to_pair:
        c.wait_send()
    for c in (w_x, w_y, w_zy, w_f1, w_f2a, w_f2b, w_da, w_db, w_f3):
        c.wait_send()
    for m in range(3):
        for c in v_copies(m):
            c.wait_send()
        for c in (v_copies(m)[2], v_copies(m)[3], v_copies(m)[6]):
            c.wait_recv()


def step_kernel(xt, dyt, w1, w3, w2, v1, v3, v2, g):
    any_spec = pl.BlockSpec(memory_space=pl.ANY)
    vmem = pl.BlockSpec(memory_space=pltpu.VMEM)
    bf, f32 = jnp.bfloat16, jnp.float32
    V = pltpu.VMEM
    dma = pltpu.SemaphoreType.DMA
    return pl.pallas_call(
        kernel,
        name='mlp_step',
        out_shape=(V((D, N), bf), V((3, D, F), f32), V((3, D, F), bf), V((3, SH, D), f32)),
        in_specs=[any_spec] * 9,
        out_specs=(vmem,) * 4,
        scratch_shapes=[
            V((NT, D, T), bf), V((2, 3, FC, D), bf), V((4, D, 3 * FC), bf),
            V((3 * FC, D), bf), V((NT, D, T), f32),
            V((2 * FC, T), bf), V((FC, T), bf), V((2 * FC, T), bf), V((FC, T), bf),
            V((4, RT, F), f32), V((6, 4, RT, FC), bf), V((6, 4, RT, FC), bf), V((6, 2, RT, FC), bf),
            V((6, RT, FC), bf), V((6, RT, FC), bf), V((6, RT, FC), f32), V((6, RT, FC), f32), V((6, RT, FC), f32),
            dma((2, NT)), dma((6,)), dma((4,)), dma((93,)), dma((93,)),
        ],
        compiler_params=pltpu.CompilerParams(
            collective_id=0, has_side_effects=True, vmem_limit_bytes=45_500_000),
        cost_estimate=pl.CostEstimate(flops=43_500_000_000, bytes_accessed=60_000_000, transcendentals=4_718_592),
    )(xt, dyt, w1, w3, w2, v1, v3, v2, g)


def solution(mesh):
    def device_step(x_loc, dy_loc, w_gate, w_up, w_down, v_gate, v_up, v_down, g_next):
        dxt, dw, vo, gs = step_kernel(
            x_loc.T, dy_loc.T, w_gate.T, w_up.T, w_down, v_gate.T, v_up.T, v_down, g_next.reshape(3 * D, F))
        return dxt.T, gs.transpose(0, 2, 1), dw[None], vo[0], vo[1], vo[2].T

    row_spec = P(ALL_AXES, None)
    col_shard = P(None, FSDP_AXES)
    row_shard = P(FSDP_AXES, None)
    dev_spec = P(ALL_AXES, None, None, None)
    return jax.shard_map(
        device_step, mesh=mesh,
        in_specs=(row_spec, row_spec, col_shard, col_shard, row_shard, col_shard, col_shard, row_shard, dev_spec),
        out_specs=(row_spec, P(None, None, FSDP_AXES), dev_spec, P(), P(), P()),
        check_vma=False)
```

```python
import functools

import jax
import jax.numpy as jnp
from jax import lax
from jax.experimental import pallas as pl
from jax.experimental.pallas import tpu as pltpu
from jax.sharding import PartitionSpec as P

ALL_AXES = ('dp', 'col', 'fsdp')
FSDP_AXES = ('col', 'fsdp')
MESH = pl.DeviceIdType.MESH

D = 576
F = 1536
N = 3072
T = 512
NT = N // T
SH = 192
FC = 384
RT = 144
HR = D // 2
QR = HR // 2
NN = (((1,), (0,)), ((), ()))
NTD = (((1,), (1,)), ((), ()))

STEPS = {
    'AX': (4, 5, 7), 'AY': (0, 1, 2), 'BX': (7, 10, 12), 'BY': (5, 6, 8), 'CX': (9, 12, 14), 'CY': (8, 11, 13),
    'W1': (4,), 'WX': (5,), 'WZ': (7,), 'WDA': (7,), 'WDB': (9,), 'W3': (16,), 'V': (13,), 'V1': (18, 19, 21), 'V2': (22, 23),
    'D0': (11, 14, 16), 'D1': (10, 13, 15), 'E0': (15, 18, 21), 'E1': (13, 16, 20),
    'F0': (18, 21, 24), 'F1': (16, 19, 23),
}


def dot(a, b, dn=NN):
    return lax.dot_general(a, b, dn, preferred_element_type=jnp.float32)


def kernel(xt, dyt, w1, w3, w2, v1, v3, v2, g, dxt, dw, vo, gs,
           ys, pair, blk, wt, dxa, dab0, hb0, dab1, hb1,
           gf, gb, gp, r1, r2, zb, z2, zs, tp,
           s_tok, s_loc, s_g, ss, rs):
    xs = dxt
    z = lax.axis_index('dp')
    y = lax.axis_index('col')
    f = lax.axis_index('fsdp')
    x = f // 2
    k = f % 2
    own = 2 * y + x
    partner = (z, y, f + 1 - 2 * k)
    xn = (z, y, (f + 2) % 4)
    yn = (z, 1 - y, f)
    z_pair = z + 1 - 2 * (z % 2)
    zp = (z_pair, y, f)
    zm = (3 - z, y, f)
    at_end = (z == 0) | (z == 3)
    inner = (z == 1) | (z == 2)

    def rcopy(n, src, dst, dev):
        return pltpu.make_async_remote_copy(
            src_ref=src, dst_ref=dst, send_sem=ss.at[n], recv_sem=rs.at[n], device_id=dev, device_id_type=MESH)

    def tok(t):
        cols = pl.ds(pl.multiple_of(t * T, T), T)
        return (pltpu.make_async_copy(xt.at[:, cols], xs.at[:, cols], s_tok.at[0, t]),
                pltpu.make_async_copy(dyt.at[:, cols], ys.at[t], s_tok.at[1, t]))

    def g_tile(o):
        return jnp.where(o < 3, o + 3, o - 3)

    def gload(n):
        own_half = n >= 6
        o = jnp.where(own_half, n - 6, n)
        i = g_tile(o)
        h = jnp.where(own_half, k, 1 - k)
        r0 = pl.multiple_of(h * (6 * RT) + i * RT, RT)
        return pltpu.make_async_copy(g.at[pl.ds(r0, RT), :], gf.at[n % 4], s_g.at[n % 4])

    shards = ((w1, w3, w2), (v1, v3, v2))
    myrows = pl.ds(pl.multiple_of(k * SH, SH), SH)
    local_shards = [pltpu.make_async_copy(shards[u][m], pair.at[u, m, myrows, :], s_loc.at[3 * u + m])
                    for u in range(2) for m in range(3)]
    for n in range(4):
        gload(n).start()
    for c in local_shards:
        c.start()

    bar = pltpu.get_barrier_semaphore()
    for dev in (partner, xn, yn, zp, zm):
        pl.semaphore_signal(bar, inc=1, device_id=dev, device_id_type=MESH)
    pl.semaphore_wait(bar, 5)

    to_pair = [rcopy(3 * u + m, shards[u][m], pair.at[u, m, myrows, :], partner) for u in range(2) for m in range(3)]
    half = pl.ds(pl.multiple_of(k * HR, HR), HR)
    other = pl.ds(pl.multiple_of((1 - k) * HR, HR), HR)
    qa = pl.ds(pl.multiple_of(k * HR, QR), QR)
    qb = pl.ds(pl.multiple_of(k * HR + QR, QR), QR)

    def blkcols(cx, cy):
        xx = 1 - x if cx else x
        yy = 1 - y if cy else y
        return pl.ds(pl.multiple_of((2 * yy + xx) * FC, FC), FC)

    zo = z % 2
    qm = pl.ds(pl.multiple_of(k * HR + zo * QR, QR), QR)
    qo = pl.ds(pl.multiple_of(k * HR + (1 - zo) * QR, QR), QR)
    w_xa = rcopy(6, blk.at[0, qa, :], blk.at[1, qa, :], xn)
    w_xb = rcopy(8, blk.at[0, qb, :], blk.at[1, qb, :], xn)
    w_y = rcopy(7, blk.at[0, qm, :], blk.at[2, qm, :], yn)
    w_zy = rcopy(9, blk.at[2, qm, :], blk.at[2, qm, :], zp)
    w_f1a = rcopy(62, blk.at[1, qa, :], blk.at[1, qa, :], partner)
    w_f1b = rcopy(63, blk.at[1, qb, :], blk.at[1, qb, :], partner)
    w_f2a = rcopy(64, blk.at[2, qm, :], blk.at[2, qm, :], partner)
    w_f2b = rcopy(65, blk.at[2, qo, :], blk.at[2, qo, :], partner)
    w_da = rcopy(10, blk.at[1, qa, :], blk.at[3, qa, :], yn)
    w_db = rcopy(11, blk.at[2, qb, :], blk.at[3, qb, :], xn)
    w_f3 = rcopy(12, blk.at[3, half, :], blk.at[3, half, :], partner)

    def v_copies(m):
        n = 66 + 7 * m
        q0, q1, q2, q3 = blkcols(0, 0), blkcols(1, 0), blkcols(0, 1), blkcols(1, 1)
        return (rcopy(n, vo.at[m, half, q0], vo.at[m, half, q0], xn),
                rcopy(n + 1, vo.at[m, half, q0], vo.at[m, half, q0], yn),
                rcopy(n + 2, vo.at[m, half, q1], vo.at[m, half, q1], partner),
                rcopy(n + 3, vo.at[m, half, q2], vo.at[m, half, q2], partner),
                rcopy(n + 4, vo.at[m, qa, q1], vo.at[m, qa, q1], yn),
                rcopy(n + 5, vo.at[m, qb, q2], vo.at[m, qb, q2], xn),
                rcopy(n + 6, vo.at[m, half, q3], vo.at[m, half, q3], partner))

    def to_partner(i):
        return rcopy(20 + i, gb.at[i], gp.at[i], partner)

    def first_x(j, yy):
        return rcopy(26 + 2 * j + yy, gp.at[j, 2 * yy + 1 - x], r1.at[j, yy], xn)

    def first_y(j, xx):
        return rcopy(32 + 2 * j + xx, gp.at[3 + j, 2 * (1 - y) + xx], r1.at[3 + j, xx], yn)

    def second_y(j):
        return rcopy(38 + j, r1.at[j, 1 - y], r2.at[j], yn)

    def second_x(j):
        return rcopy(41 + j, r1.at[3 + j, 1 - x], r2.at[3 + j], xn)

    def z_in(i):
        return rcopy(44 + i, zb.at[i], zb.at[i], zp)

    def z_mid(i):
        return rcopy(50 + i, zs.at[i], z2.at[i], zm)

    def z_out(i):
        return rcopy(56 + i, z2.at[i], z2.at[i], zp)

    def t_pair(i):
        return rcopy(87 + i, z2.at[i], tp.at[i], partner)

    for c in to_pair:
        c.start()
    for c in tok(0):
        c.start()

    def send_half(n, _):
        i = g_tile(n)
        gload(n).wait()
        for q in range(4):
            gb[i, q] = gf[n % 4, :, q * FC:(q + 1) * FC].astype(jnp.bfloat16)
        to_partner(i).start()
        gload(n + 4).start()
        return 0

    lax.fori_loop(0, 2, send_half, 0)

    for m in range(3):
        local_shards[m].wait()
        to_pair[m].wait_recv()
        blk[0, :, m * FC:(m + 1) * FC] = pair[0, m].T
    w_xa.start()
    w_xb.start()
    w_y.start()
    lax.fori_loop(2, 6, send_half, 0)
    for t in range(1, NT):
        for c in tok(t):
            c.start()

    def own_tile(i):
        n = 6 + (3, 4, 5, 0, 1, 2)[i]
        gload(n).wait()
        to_partner(i).wait_recv()
        for q in range(4):
            gp[i, q] = (gp[i, q].astype(jnp.float32)
                        + gf[n % 4, :, q * FC:(q + 1) * FC].astype(jnp.bfloat16).astype(jnp.float32)
                        ).astype(jnp.bfloat16)
        if n + 4 < 12:
            gload(n + 4).start()

    def stage_ax(j):
        own_tile(j)
        for b in range(2):
            first_x(j, b).start()

    def stage_ay(j):
        own_tile(3 + j)
        for b in range(2):
            first_y(j, b).start()

    def stage_bx(j):
        for b in range(2):
            first_x(j, b).wait_recv()
            r1[j, b] = (gp[j, 2 * b + x].astype(jnp.float32) + r1[j, b].astype(jnp.float32)).astype(jnp.bfloat16)
        second_y(j).start()

    def stage_by(j):
        for b in range(2):
            first_y(j, b).wait_recv()
            r1[3 + j, b] = (gp[3 + j, 2 * y + b].astype(jnp.float32)
                            + r1[3 + j, b].astype(jnp.float32)).astype(jnp.bfloat16)
        second_x(j).start()

    def second(i):
        return second_y(i) if i < 3 else second_x(i - 3)

    def mine(i):
        return y if i < 3 else x

    def stage_c(i):
        @pl.when(at_end)
        def _():
            second(i).wait_recv()
            zb[i] = (r1[i, mine(i)].astype(jnp.float32) + r2[i].astype(jnp.float32)).astype(jnp.bfloat16)
            z_in(i).start()

    def stage_d(i):
        @pl.when(inner)
        def _():
            second(i).wait_recv()
            z_in(i).wait_recv()
            zs[i] = (r1[i, mine(i)].astype(jnp.float32) + r2[i].astype(jnp.float32)) + zb[i].astype(jnp.float32)
            z_mid(i).start()

    def stage_e(i):
        @pl.when(inner)
        def _():
            z_mid(i).wait_recv()
            z2[i] = zs[i] + z2[i]
            z_out(i).start()
            t_pair(i).start()

    def stage_f(i):
        @pl.when(at_end)
        def _():
            z_out(i).wait_recv()
            t_pair(i).start()

    def v_turn():
        for m in range(3):
            local_shards[3 + m].wait()
            to_pair[3 + m].wait_recv()
            vo[m, :, blkcols(0, 0)] = pair[1, m].T

    def v_start():
        for m in range(3):
            v_copies(m)[0].start()
            v_copies(m)[1].start()

    def w_1():
        w_y.wait_recv()
        w_zy.start()
        w_f2a.start()

    def w_xf():
        w_xa.wait_recv()
        w_f1a.start()

    def w_z():
        w_zy.wait_recv()
        w_f2b.start()

    def w_3():
        w_da.wait_recv()
        w_db.wait_recv()
        w_f3.start()

    def v_1(m):
        v_x, v_y, v_f1, v_f2, v_da, v_db, _ = v_copies(m)
        v_x.wait_recv()
        v_da.start()
        v_f1.start()
        v_y.wait_recv()
        v_db.start()
        v_f2.start()

    def v_2(m):
        v_da, v_db, v_f3 = v_copies(m)[4:]
        v_da.wait_recv()
        v_db.wait_recv()
        v_f3.start()

    stages = {
        'AX': stage_ax, 'AY': stage_ay, 'BX': stage_bx, 'BY': stage_by,
        'CX': stage_c, 'CY': lambda j: stage_c(3 + j),
        'D0': stage_d, 'D1': lambda j: stage_d(3 + j), 'E0': stage_e, 'E1': lambda j: stage_e(3 + j),
        'F0': stage_f, 'F1': lambda j: stage_f(3 + j), 'V': lambda j: v_start(), 'V1': v_1, 'V2': v_2,
        'W1': lambda j: w_1(), 'WX': lambda j: w_xf(), 'WZ': lambda j: w_z(), 'WDA': lambda j: w_da.start(), 'WDB': lambda j: w_db.start(),
        'W3': lambda j: w_3(),
    }
    order = ('W1', 'WX', 'WZ', 'W3', 'BX', 'BY', 'AX', 'AY', 'CX', 'CY', 'D0', 'D1', 'E0', 'E1', 'F0', 'F1', 'WDA', 'WDB', 'V', 'V1', 'V2')

    def tick(step, steps):
        for name in order:
            for j, n in enumerate(STEPS[name]):
                if n in steps:
                    if len(steps) == 1:
                        stages[name](j)
                    else:
                        pl.when(step == n)(functools.partial(stages[name], j))

    def dw_cols(c):
        cx, cy = c % 2, c // 2
        q = 2 * (y + cy - 2 * y * cy) + x + cx - 2 * x * cx
        return pl.ds(pl.multiple_of(q * FC, FC), FC)

    def head(c):
        dw[:, :, dw_cols(c)] = jnp.zeros((3, D, FC), jnp.float32)

        @pl.when(c == 1)
        def _():
            w_xb.wait_recv()
            w_f1b.start()
            v_turn()
            w_f1a.wait_recv()
            w_f1b.wait_recv()

        @pl.when(c == 2)
        def _():
            w_f2a.wait_recv()
            w_f2b.wait_recv()

        @pl.when(c == 3)
        def _():
            w_f3.wait_recv()

        for m in range(3):
            rows = slice(m * FC, (m + 1) * FC)
            wt[rows, :] = pair[0, m] if isinstance(c, int) else blk[c, :, rows].T

    def first_touch(t):
        for cp in tok(t):
            cp.wait()
        dxa[t] = jnp.zeros((D, T), jnp.float32)

    def tcols(t):
        return pl.ds(pl.multiple_of(t * T, T), T)

    def forward(t, dab, hb):
        xv = xs[:, tcols(t)]
        a = dot(wt[0:FC, :], xv)
        b = dot(wt[FC:2 * FC, :], xv)
        dh = dot(wt[2 * FC:3 * FC, :], ys[t])
        sg = jnp.tanh(a * 0.5) * 0.5 + 0.5
        act = a * sg
        hb[...] = (act * b).astype(jnp.bfloat16)
        dab[FC:, :] = (dh * act).astype(jnp.bfloat16)
        dab[:FC, :] = (dh * b * (sg + act * (1.0 - sg))).astype(jnp.bfloat16)

    def backward(step, dab, hb):
        c, t = step // NT, step % NT
        dxa[t] += dot(blk[c, :, :2 * FC], dab[...])
        gw = dot(xs[:, tcols(t)], dab[...], NTD)
        cols = dw_cols(c)
        dw[0, :, cols] += gw[:, :FC]
        dw[1, :, cols] += gw[:, FC:]
        dw[2, :, cols] += dot(ys[t], hb[...], NTD)

    def half_step(step, steps, src, dst):
        c, t = step // NT, step % NT
        if any(n % NT == 0 for n in steps):
            @pl.when(t == 0)
            def _():
                head(c)

        if any(n < NT for n in steps):
            @pl.when(c == 0)
            def _():
                first_touch(t)

        tick(step, steps)
        forward(t, *dst)
        backward(step - 1, *src)

    b0, b1 = (dab0, hb0), (dab1, hb1)
    head(0)
    first_touch(0)
    tick(0, (0,))
    forward(0, *b0)

    def two_steps(p, _):
        half_step(2 * p + 1, tuple(range(1, 23, 2)), b0, b1)
        half_step(2 * p + 2, tuple(range(2, 23, 2)), b1, b0)
        return 0

    lax.fori_loop(0, 11, two_steps, 0)
    half_step(23, (23,), b0, b1)
    v_2(2)
    backward(23, *b1)

    def write_dx(t, _):
        xs[:, tcols(t)] = dxa[t].astype(jnp.bfloat16)
        return 0

    lax.fori_loop(0, NT, write_dx, 0)

    for name in order:
        for j, n in enumerate(STEPS[name]):
            if n >= 24:
                stages[name](j)

    for i in range(6):
        t_pair(i).wait_recv()

    for m in range(3):
        for kk in range(2):
            @pl.when(k == kk)
            def _():
                tiles = []
                for r in range(4 * m, 4 * m + 4):
                    src = z2 if r // 6 == kk else tp
                    tiles.append(src[r % 6])
                full = jnp.concatenate(tiles, axis=0).T
                gs[m] = full[kk * SH:(kk + 1) * SH]

    for i in range(6):
        t_pair(i).wait_send()
        to_partner(i).wait_send()

        @pl.when(at_end)
        def _():
            z_in(i).wait_send()

        @pl.when(inner)
        def _():
            z_mid(i).wait_send()
            z_out(i).wait_send()
    for j in range(3):
        for b in range(2):
            first_x(j, b).wait_send()
            first_y(j, b).wait_send()
        second_x(j).wait_send()
        second_y(j).wait_send()
    for c in to_pair:
        c.wait_send()
    for c in (w_xa, w_xb, w_y, w_zy, w_f1a, w_f1b, w_f2a, w_f2b, w_da, w_db, w_f3):
        c.wait_send()
    for m in range(3):
        for c in v_copies(m):
            c.wait_send()
        for c in (v_copies(m)[2], v_copies(m)[3], v_copies(m)[6]):
            c.wait_recv()


def step_kernel(xt, dyt, w1, w3, w2, v1, v3, v2, g):
    any_spec = pl.BlockSpec(memory_space=pl.ANY)
    vmem = pl.BlockSpec(memory_space=pltpu.VMEM)
    bf, f32 = jnp.bfloat16, jnp.float32
    V = pltpu.VMEM
    dma = pltpu.SemaphoreType.DMA
    return pl.pallas_call(
        kernel,
        name='mlp_step',
        out_shape=(V((D, N), bf), V((3, D, F), f32), V((3, D, F), bf), V((3, SH, D), f32)),
        in_specs=[any_spec] * 9,
        out_specs=(vmem,) * 4,
        scratch_shapes=[
            V((NT, D, T), bf), V((2, 3, FC, D), bf), V((4, D, 3 * FC), bf),
            V((3 * FC, D), bf), V((NT, D, T), f32),
            V((2 * FC, T), bf), V((FC, T), bf), V((2 * FC, T), bf), V((FC, T), bf),
            V((4, RT, F), f32), V((6, 4, RT, FC), bf), V((6, 4, RT, FC), bf), V((6, 2, RT, FC), bf),
            V((6, RT, FC), bf), V((6, RT, FC), bf), V((6, RT, FC), f32), V((6, RT, FC), f32), V((6, RT, FC), f32),
            dma((2, NT)), dma((6,)), dma((4,)), dma((93,)), dma((93,)),
        ],
        compiler_params=pltpu.CompilerParams(
            collective_id=0, has_side_effects=True, vmem_limit_bytes=45_500_000),
        cost_estimate=pl.CostEstimate(flops=43_500_000_000, bytes_accessed=60_000_000, transcendentals=4_718_592),
    )(xt, dyt, w1, w3, w2, v1, v3, v2, g)


def solution(mesh):
    def device_step(x_loc, dy_loc, w_gate, w_up, w_down, v_gate, v_up, v_down, g_next):
        dxt, dw, vo, gs = step_kernel(
            x_loc.T, dy_loc.T, w_gate.T, w_up.T, w_down, v_gate.T, v_up.T, v_down, g_next.reshape(3 * D, F))
        return dxt.T, gs.transpose(0, 2, 1), dw[None], vo[0], vo[1], vo[2].T

    row_spec = P(ALL_AXES, None)
    col_shard = P(None, FSDP_AXES)
    row_shard = P(FSDP_AXES, None)
    dev_spec = P(ALL_AXES, None, None, None)
    return jax.shard_map(
        device_step, mesh=mesh,
        in_specs=(row_spec, row_spec, col_shard, col_shard, row_shard, col_shard, col_shard, row_shard, dev_spec),
        out_specs=(row_spec, P(None, None, FSDP_AXES), dev_spec, P(), P(), P()),
        check_vma=False)
```
